32 devices in a mesh: sys: 1 (over z), aux: 4 (over y), orb: 8 (over x, core).
Axes of the slice: x: 4, y: 4, z: 1, core: 2. Of those that a mesh axis runs over, the one named last changes fastest.
The devices are a block of a 4x4x8 slice.
Arguments:
- fit_tensor: float32 [1160, 240, 240], P(('sys', 'aux'), 'orb')
- occ_orbitals: float32 [240, 50], P('sys')
Outputs:
- output: float32 [240, 240], P(('sys', 'orb'), 'aux')
All inputs are finite; a program needn't handle non-finite values.
Results may differ from the reference program's by a relative error of at most 0.001.
Values are sent between devices in bfloat16 or wider.
A program may use at most 768 MiB of HBM per device.

```python
import math
import jax
import jax.numpy as jnp
from jax import lax

NBF = 240
NOCC = 50
NAUX = 1160

PREC_MODE = lax.Precision.HIGHEST


def setup_inputs(seed: int = 0, part: int = 0) -> dict:
    root_key = jax.random.fold_in(jax.random.key(seed), part)
    key_orb, key_dir, key_wgt, key_noise = jax.random.split(root_key, 4)
    orbitals = jnp.linalg.qr(jax.random.normal(key_orb, (NBF, NOCC), jnp.float32))[0]
    n_groups = 64
    directions = jax.random.normal(key_dir, (n_groups, NBF), jnp.float32)
    weights = jax.random.normal(key_wgt, (NAUX,), jnp.float32)
    group_of = jnp.arange(NAUX) * n_groups // NAUX
    noise_keys = jax.random.split(key_noise, NAUX)
    noise_scale = math.sqrt(math.sqrt(n_groups) / (NAUX * NOCC))

    def one_aux(packed):
        aux_key, weight, grp_index = packed
        noise_mat = jax.random.normal(aux_key, (NBF, NBF), jnp.float32)
        direction = directions[grp_index]
        sym_noise = (noise_mat + noise_mat.T) * math.sqrt(0.5)
        return noise_scale * (sym_noise + weight * jnp.outer(direction, direction))

    fit_tensor = lax.map(one_aux, (noise_keys, weights, group_of))
    return {'fit_tensor': fit_tensor, 'occ_orbitals': orbitals}


def reference(fit_tensor, occ_orbitals):
    density = jnp.dot(occ_orbitals, occ_orbitals.T, precision=PREC_MODE, preferred_element_type=jnp.float32)
    fit_flat = fit_tensor.reshape(NAUX, NBF * NBF)
    aux_coef = jnp.dot(fit_flat, density.reshape(NBF * NBF), precision=PREC_MODE, preferred_element_type=jnp.float32)
    coulomb = jnp.dot(aux_coef, fit_flat, precision=PREC_MODE, preferred_element_type=jnp.float32).reshape(NBF, NBF)
    half_t = jnp.dot(fit_tensor.reshape(NAUX * NBF, NBF), occ_orbitals, precision=PREC_MODE, preferred_element_type=jnp.float32).reshape(NAUX, NBF, NOCC)
    exchange = jnp.einsum('qmi,qni->mn', half_t, half_t, precision=PREC_MODE, preferred_element_type=jnp.float32)
    return 2.0 * coulomb - exchange
```

```python
import functools
import jax
import jax.numpy as jnp
from jax import lax
from jax.experimental import pallas as pl
from jax.experimental.pallas import tpu as pltpu
from jax.sharding import PartitionSpec as P

PREC_MODE = lax.Precision.HIGHEST
MESH_ID = pl.DeviceIdType.MESH
LANES = 128
SUBL = 8


def mm(lhs, rhs, lhs_dim, rhs_dim):
    return lax.dot_general(lhs, rhs, (((lhs_dim,), (rhs_dim,)), ((), ())), precision=PREC_MODE, preferred_element_type=jnp.float32)


def rup(value, unit):
    return -(-value // unit) * unit


def fock_kernel(dims, fit_ref, occ_ref, out_ref, bv, ct, dens, recv, send, ex_send, ex_recv, xs, kacc,
                srow, gsend, grecv, gbc, jsend, jrecv, ksend, krecv,
                load_sem, t_ss, t_rs, l_ss, l_rs, g_ss, g_rs, j_ss, j_rs, k_ss, k_rs):
    n_orb, n_aux, q_loc, row_blk, n_bf, n_occ, row_pad, occ_pad, occ_main, q_tile, rounds, q_left, left_base, left_row, n_cols = dims
    me = lax.axis_index('orb')
    my = lax.axis_index('aux')
    n_dev = n_orb * n_aux

    def peer_orb(step):
        return lax.rem(me + step, n_orb)

    def loads():
        for rd, (q_base, tiles, t_base) in enumerate(rounds):
            size = tiles * q_tile * n_orb + (q_left if rd == len(rounds) - 1 else 0)
            yield pltpu.make_async_copy(fit_ref.at[pl.ds(q_base, size)], bv.at[pl.ds(q_base, size)], load_sem.at[rd])

    load_list = list(loads())
    for cp in load_list:
        cp.start()

    ex_send[...] = jnp.zeros(ex_send.shape, jnp.float32)
    ex_recv[me] = jnp.zeros(ex_recv.shape[1:], jnp.float32)
    barrier = pltpu.get_barrier_semaphore()

    def greet(step, carry):
        pl.semaphore_signal(barrier, inc=1, device_id={'orb': lax.rem(me + lax.rem(step, n_orb), n_orb), 'aux': lax.rem(my + step // n_orb, n_aux)}, device_id_type=MESH_ID)
        return carry

    lax.fori_loop(1, n_dev, greet, 0)

    occ = occ_ref[...]

    def rows_of_ct(count, scale, shift):
        row = lax.broadcasted_iota(jnp.int32, (count, n_occ), 0)
        col = lax.broadcasted_iota(jnp.int32, (count, n_occ), 1)
        return mm((row * scale + shift == col).astype(jnp.float32), occ, 1, 1)

    half_occ = rup(n_occ, 2 * SUBL) // 2
    ct[0:occ_pad, :] = rows_of_ct(occ_pad, 1, 0)
    ct[occ_pad:occ_pad + half_occ, :] = rows_of_ct(half_occ, 2, 0)
    ct[occ_pad + half_occ:, :] = rows_of_ct(half_occ, 2, 1)
    pick = lax.broadcasted_iota(jnp.int32, (row_blk, n_bf), 0)
    pick_col = lax.broadcasted_iota(jnp.int32, (row_blk, n_bf), 1)
    own = mm((pick + me * row_blk == pick_col).astype(jnp.float32), occ, 1, 0)
    dens[...] = mm(own, occ, 1, 1)

    n_rounds = len(rounds)

    def t_copy(rd, dst, src_dev):
        q_base, tiles, t_base = rounds[rd]
        return pltpu.make_async_remote_copy(
            src_ref=send.at[dst, pl.ds(t_base, tiles)],
            dst_ref=recv.at[src_dev, pl.ds(t_base, tiles)],
            send_sem=t_ss.at[rd, dst], recv_sem=t_rs.at[rd, src_dev],
            device_id={'orb': dst}, device_id_type=MESH_ID)

    def padded_rows(q_start, n_q):
        block = bv[pl.ds(q_start, n_q)]
        block = jnp.concatenate([block, jnp.zeros((n_q, row_pad - row_blk, n_bf), jnp.float32)], axis=1)
        return block.reshape(n_q * row_pad, n_bf)

    def t_block(rd, dst, into, into_ex):
        q_base, tiles, t_base = rounds[rd]
        n_q = tiles * q_tile
        block = mm(ct[0:occ_pad, :], padded_rows(q_base + dst * n_q, n_q), 1, 1)
        extra = n_occ - occ_main
        for tile in range(tiles):
            piece = block[:, tile * LANES:(tile + 1) * LANES]
            into[dst, t_base + tile] = piece[0:occ_main]
            at = (t_base + tile) * extra
            into_ex[dst, at:at + extra, :] = piece[occ_main:n_occ]

    def t_round(rd, first):
        q_base, tiles, t_base = rounds[rd]
        load_list[rd].wait()

        def step(r, carry):
            dst = peer_orb(r)
            t_block(rd, dst, send, ex_send)

            @pl.when(r > 1)
            def _():
                t_copy(rd, peer_orb(r - 1), me).start()
            return carry

        if first:
            step(1, 0)
            pl.semaphore_wait(barrier, n_dev - 1)
            lax.fori_loop(2, n_orb, step, 0)
        else:
            lax.fori_loop(1, n_orb, step, 0)
        t_block(rd, me, recv, ex_recv)
        t_copy(rd, peer_orb(n_orb - 1), me).start()

    def l_copy(dst, src_dev):
        return pltpu.make_async_remote_copy(
            src_ref=ex_send.at[dst], dst_ref=ex_recv.at[src_dev], send_sem=l_ss.at[dst], recv_sem=l_rs.at[src_dev],
            device_id={'orb': dst}, device_id_type=MESH_ID)

    def g_copy(dst, src_dev):
        return pltpu.make_async_remote_copy(
            src_ref=gsend, dst_ref=grecv.at[src_dev], send_sem=g_ss.at[dst], recv_sem=g_rs.at[src_dev],
            device_id={'orb': dst}, device_id_type=MESH_ID)

    def j_copy(dst, src_dev):
        return pltpu.make_async_remote_copy(
            src_ref=jsend.at[dst], dst_ref=jrecv.at[src_dev], send_sem=j_ss.at[dst], recv_sem=j_rs.at[src_dev],
            device_id={'aux': dst}, device_id_type=MESH_ID)

    def k_copy(orb, aux, src_dev):
        slot = aux * n_orb + orb
        return pltpu.make_async_remote_copy(
            src_ref=ksend.at[slot], dst_ref=krecv.at[src_dev], send_sem=k_ss.at[slot], recv_sem=k_rs.at[src_dev],
            device_id={'orb': orb, 'aux': aux}, device_id_type=MESH_ID)

    def gamma_part():
        for cp in load_list[2:]:
            cp.wait()

        def body(q, carry):
            srow[pl.ds(q, 1), :] = jnp.sum(bv[q] * dens[...], axis=0, keepdims=True)
            return carry

        lax.fori_loop(0, q_loc, body, 0, unroll=10)
        total = jnp.zeros((SUBL, LANES), jnp.float32)
        for k in range(srow.shape[0] // LANES):
            row_k = (lax.broadcasted_iota(jnp.int32, (SUBL, n_bf), 0) == k).astype(jnp.float32)
            total = total + mm(row_k, srow[k * LANES:(k + 1) * LANES, :], 1, 1)
        gsend[...] = total
        grecv[me] = total

    def gamma_send():
        for r in range(1, n_orb):
            g_copy(peer_orb(r), me).start()

    def coulomb():
        for r in range(1, n_orb):
            g_copy(me, peer_orb(r)).wait_recv()
        gam = grecv[0]
        for src in range(1, n_orb):
            gam = gam + grecv[src]
        for k in range(srow.shape[0] // LANES):
            row_k = (lax.broadcasted_iota(jnp.int32, (SUBL, n_bf), 0) == k).astype(jnp.float32)
            gbc[k * LANES:(k + 1) * LANES, :] = mm(gam, row_k, 0, 0)

        def body(q, acc):
            return acc + bv[q] * gbc[pl.ds(q, 1), :]

        jfull = lax.fori_loop(0, q_loc, body, jnp.zeros((row_blk, n_bf), jnp.float32), unroll=10)
        jpad = jnp.concatenate([jfull, jnp.zeros((row_blk, 2 * LANES - n_bf), jnp.float32)], axis=1)
        for a in range(n_aux):
            piece = jpad if a == 0 else pltpu.roll(jpad, 2 * LANES - a * n_cols, 1)
            jsend[a, 0:row_blk, :] = piece[:, 0:LANES]
        jrecv[my] = jsend[my]
        for r in range(1, n_aux):
            j_copy(lax.rem(my + r, n_aux), my).start()

    lane = lax.broadcasted_iota(jnp.int32, (occ_main, LANES), 1)

    def regroup(parts):
        rows = parts[0].shape[0]
        ln = lane[0:rows]
        low = ln < 2 * row_pad
        even = (ln // row_pad) % 2 == 0
        a0, a1, a2, a3 = parts
        b0 = jnp.where(low, a0, pltpu.roll(a2, 2 * row_pad, 1))
        b2 = jnp.where(low, pltpu.roll(a0, 2 * row_pad, 1), a2)
        b1 = jnp.where(low, a1, pltpu.roll(a3, 2 * row_pad, 1))
        b3 = jnp.where(low, pltpu.roll(a1, 2 * row_pad, 1), a3)
        back = LANES - row_pad
        return [jnp.where(even, b0, pltpu.roll(b1, row_pad, 1)), jnp.where(even, pltpu.roll(b0, back, 1), b1),
                jnp.where(even, b2, pltpu.roll(b3, row_pad, 1)), jnp.where(even, pltpu.roll(b2, back, 1), b3)]

    def exchange_round(rd):
        q_base, tiles, t_base = rounds[rd]
        last = rd == n_rounds - 1
        for r in range(1, n_orb):
            t_copy(rd, me, peer_orb(r)).wait_recv()
        if last:
            for r in range(1, n_orb):
                l_copy(me, peer_orb(r)).wait_recv()
        depth = tiles * q_tile * occ_main
        n_ex = ex_recv.shape[1]
        for grp in range(n_orb // q_tile):
            cols = slice(grp * LANES, (grp + 1) * LANES)
            for tile in range(tiles):
                outs = regroup([recv[grp * q_tile + j, t_base + tile] for j in range(q_tile)])
                for q in range(q_tile):
                    base = (tile * q_tile + q) * occ_main
                    xs[base:base + occ_main, cols] = outs[q]
            if last:
                outs = regroup([ex_recv[grp * q_tile + j] for j in range(q_tile)])
                for q in range(q_tile):
                    xs[depth + q * n_ex:depth + (q + 1) * n_ex, cols] = outs[q]
        if last:
            depth += q_tile * n_ex
        xv = xs[0:depth, :]
        part = mm(xv, xv, 0, 0)
        kacc[...] = part if rd == 0 else kacc[...] + part

    t_round(0, True)
    t_round(1, False)
    gamma_part()
    class Done:
        def wait(self):
            pass
    for rd in range(2, n_rounds):
        load_list[rd] = Done()
    t_round(2, False)
    gamma_send()
    t_round(3, False)
    coulomb()
    t_round(4, False)
    left_rows = padded_rows(left_base, q_left)
    left_rows = jnp.concatenate([left_rows, left_rows], axis=0)
    first = lax.broadcasted_iota(jnp.int32, (half_occ, LANES), 1) < LANES // 2
    left = jnp.where(first, mm(ct[occ_pad:occ_pad + half_occ, :], left_rows, 1, 1), mm(ct[occ_pad + half_occ:, :], left_rows, 1, 1))
    share = half_occ // n_orb
    for dst in range(n_orb):
        ex_send[dst, left_row:left_row + share, :] = left[dst * share:(dst + 1) * share, :]
    ex_recv[me, left_row:left_row + share, :] = ex_send[me, left_row:left_row + share, :]
    exchange_round(0)
    for r in range(1, n_orb):
        l_copy(peer_orb(r), me).start()
    for rd in range(1, n_rounds):
        exchange_round(rd)

    half = row_pad // 2
    low_half = lax.broadcasted_iota(jnp.int32, (half, LANES), 1) < LANES // 2
    for orb in range(n_orb):
        for ctile in range(n_aux // 2):
            blk = kacc[orb * row_pad:(orb + 1) * row_pad, ctile * LANES:(ctile + 1) * LANES]
            top, bot = blk[0:half], blk[half:]
            ksend[2 * ctile * n_orb + orb] = jnp.where(low_half, top, pltpu.roll(bot, LANES // 2, 1))
            ksend[(2 * ctile + 1) * n_orb + orb] = jnp.where(low_half, pltpu.roll(top, LANES // 2, 1), bot)
    dev = my * n_orb + me
    krecv[dev] = ksend[dev]

    def k_send(step, carry):
        k_copy(lax.rem(me + lax.rem(step, n_orb), n_orb), lax.rem(my + step // n_orb, n_aux), dev).start()
        return carry

    lax.fori_loop(1, n_dev, k_send, 0)
    for r in range(1, n_aux):
        j_copy(my, lax.rem(my + r, n_aux)).wait_recv()
    jsum = jrecv[0]
    for src in range(1, n_aux):
        jsum = jsum + jrecv[src]

    def k_wait(step, carry):
        src = lax.rem(my + step // n_orb, n_aux) * n_orb + lax.rem(me + lax.rem(step, n_orb), n_orb)
        k_copy(me, my, src).wait_recv()
        return carry

    lax.fori_loop(1, n_dev, k_wait, 0)
    ksum = krecv[0]
    for src in range(1, n_dev):
        ksum = ksum + krecv[src]
    kblk = jnp.concatenate([ksum, pltpu.roll(ksum, LANES // 2, 1)], axis=0)
    pad_cols = row_pad - row_blk
    kcols = jnp.where(lax.broadcasted_iota(jnp.int32, (row_pad, LANES), 1) < row_blk, kblk, pltpu.roll(kblk, LANES - pad_cols, 1))
    out = 2.0 * jsum - kcols
    out_ref[...] = out[0:row_blk, 0:n_cols]

    for rd in range(n_rounds):
        for r in range(1, n_orb):
            t_copy(rd, peer_orb(r), me).wait_send()
    for r in range(1, n_orb):
        l_copy(peer_orb(r), me).wait_send()
        g_copy(peer_orb(r), me).wait_send()
    for r in range(1, n_aux):
        j_copy(lax.rem(my + r, n_aux), my).wait_send()

    def k_drain(step, carry):
        k_copy(lax.rem(me + lax.rem(step, n_orb), n_orb), lax.rem(my + step // n_orb, n_aux), dev).wait_send()
        return carry

    lax.fori_loop(1, n_dev, k_drain, 0)


def solution(mesh):
    n_orb = mesh.shape['orb']
    n_aux = mesh.shape['aux']

    def local_fock(fit_loc, orbitals):
        q_loc, row_blk, n_bf = fit_loc.shape
        n_occ = orbitals.shape[1]
        n_cols = n_bf // n_aux
        row_pad = 32
        q_tile = LANES // row_pad
        occ_pad = rup(n_occ, SUBL)
        occ_main = n_occ // SUBL * SUBL
        all_tiles = q_loc // (q_tile * n_orb)
        rounds, q_base, t_base = [], 0, 0
        while t_base < all_tiles:
            tiles = min(2, all_tiles - t_base)
            rounds.append((q_base, tiles, t_base))
            q_base += tiles * q_tile * n_orb
            t_base += tiles
        q_left = q_loc - q_base
        left_row = all_tiles * (n_occ - occ_main)
        half_occ = rup(n_occ, 2 * SUBL) // 2
        ex_rows = rup(left_row + half_occ // n_orb, SUBL)
        assert row_blk <= row_pad and n_orb % q_tile == 0 and n_orb == 2 * n_aux and n_cols == 2 * row_blk
        assert 2 * q_left == q_tile and occ_main < n_occ and half_occ % n_orb == 0
        dims = (n_orb, n_aux, q_loc, row_blk, n_bf, n_occ, row_pad, occ_pad, occ_main, q_tile, tuple(rounds), q_left, q_base, left_row, n_cols)
        n_dev = n_orb * n_aux
        n_rounds = len(rounds)
        q_lanes = rup(q_loc, LANES)
        depth_max = max(2 * q_tile * occ_main, q_tile * (occ_main + ex_rows))
        f32 = jnp.float32
        dma = pltpu.SemaphoreType.DMA
        scratch = [
            pltpu.VMEM((q_loc, row_blk, n_bf), f32),
            pltpu.VMEM((occ_pad + 2 * half_occ, n_bf), f32),
            pltpu.VMEM((row_blk, n_bf), f32),
            pltpu.VMEM((n_orb, all_tiles, occ_main, LANES), f32),
            pltpu.VMEM((n_orb, all_tiles, occ_main, LANES), f32),
            pltpu.VMEM((n_orb, ex_rows, LANES), f32),
            pltpu.VMEM((n_orb, ex_rows, LANES), f32),
            pltpu.VMEM((depth_max, n_orb * row_pad), f32),
            pltpu.VMEM((n_orb * row_pad, n_orb * row_pad), f32),
            pltpu.VMEM((q_lanes, n_bf), f32),
            pltpu.VMEM((SUBL, LANES), f32),
            pltpu.VMEM((n_orb, SUBL, LANES), f32),
            pltpu.VMEM((q_lanes, n_bf), f32),
            pltpu.VMEM((n_aux, row_pad, LANES), f32),
            pltpu.VMEM((n_aux, row_pad, LANES), f32),
            pltpu.VMEM((n_dev, row_pad // 2, LANES), f32),
            pltpu.VMEM((n_dev, row_pad // 2, LANES), f32),
            dma((n_rounds,)), dma((n_rounds, n_orb)), dma((n_rounds, n_orb)), dma((n_orb,)), dma((n_orb,)),
            dma((n_orb,)), dma((n_orb,)), dma((n_aux,)), dma((n_aux,)), dma((n_dev,)), dma((n_dev,)),
        ]
        return pl.pallas_call(
            functools.partial(fock_kernel, dims),
            out_shape=jax.ShapeDtypeStruct((row_blk, n_cols), f32),
            in_specs=[pl.BlockSpec(memory_space=pl.ANY), pl.BlockSpec(memory_space=pltpu.VMEM)],
            out_specs=pl.BlockSpec(memory_space=pltpu.VMEM),
            scratch_shapes=scratch,
            compiler_params=pltpu.CompilerParams(collective_id=0, has_side_effects=True, vmem_limit_bytes=48 * 1024 * 1024),
            name='fock_build',
        )(fit_loc, orbitals)

    spec_fit = P(('sys', 'aux'), 'orb', None)
    spec_orbitals = P('sys', None)
    spec_out = P(('sys', 'orb'), 'aux')
    return jax.shard_map(local_fock, mesh=mesh, in_specs=(spec_fit, spec_orbitals), out_specs=spec_out, check_vma=False)
```

```python
import functools
import jax
import jax.numpy as jnp
from jax import lax
from jax.experimental import pallas as pl
from jax.experimental.pallas import tpu as pltpu
from jax.sharding import PartitionSpec as P

PREC_MODE = lax.Precision.HIGHEST
MESH_ID = pl.DeviceIdType.MESH
LANES = 128
SUBL = 8


ORDER = (4, 2, 6, 5, 3, 7, 1)


def mm(lhs, rhs, lhs_dim, rhs_dim):
    return lax.dot_general(lhs, rhs, (((lhs_dim,), (rhs_dim,)), ((), ())), precision=PREC_MODE, preferred_element_type=jnp.float32)


def rup(value, unit):
    return -(-value // unit) * unit


class Loaded:
    def wait(self):
        pass


def fock_kernel(dims, fit_ref, occ_ref, out_ref, bv, ct, ctp, ctl, dens, recv, send, ex_recv, ex_send, xa, kacc,
                srow, gsend, grecv, gbc, jrows, jsend, jrecv, ksend, krecv,
                load_sem, t_ss, t_rs, l_ss, l_rs, g_ss, g_rs, j_ss, j_rs, k_ss, k_rs):
    (n_orb, n_aux, q_loc, row_blk, n_bf, n_occ, row_pad, occ_each, groups, q_main, left_pad, fold, n_cols) = dims
    me = lax.axis_index('orb')
    my = lax.axis_index('aux')
    n_dev = n_orb * n_aux
    n_tiles = q_main // LANES
    slots = n_tiles * occ_each
    n_groups = len(groups)
    q_left = q_loc - q_main
    whole = row_blk // SUBL * SUBL
    rest = row_blk - whole
    pairs = occ_each // fold
    extra = n_occ - n_orb * occ_each

    def peer_orb(step):
        return lax.rem(me + step, n_orb)

    occ_load = pltpu.make_async_copy(occ_ref, ct, load_sem.at[n_groups])
    occ_load.start()
    load_list = [pltpu.make_async_copy(fit_ref.at[pl.ds(m0, mg)], bv.at[pl.ds(m0, mg)], load_sem.at[g]) for g, (m0, mg, base) in enumerate(groups)]
    for cp in load_list:
        cp.start()

    barrier = pltpu.get_barrier_semaphore()

    def greet(step, carry):
        pl.semaphore_signal(barrier, inc=1, device_id={'orb': lax.rem(me + lax.rem(step, n_orb), n_orb), 'aux': lax.rem(my + step // n_orb, n_aux)}, device_id_type=MESH_ID)
        return carry

    lax.fori_loop(1, n_dev, greet, 0)
    ex_send[...] = jnp.zeros(ex_send.shape, jnp.float32)

    occ_load.wait()
    occ_t = ct[...]

    def rows_of_ct(which):
        return mm(which.astype(jnp.float32), occ_t, 1, 0)

    row = lax.broadcasted_iota(jnp.int32, (n_orb * SUBL, n_occ), 0)
    col = lax.broadcasted_iota(jnp.int32, (n_orb * SUBL, n_occ), 1)
    in_blk = row % SUBL
    ctp[...] = rows_of_ct(((in_blk < occ_each) & (col == row // SUBL * occ_each + in_blk))
                          | ((in_blk == occ_each) & (col == n_orb * occ_each + row // SUBL % extra)))
    rows_l = ctl.shape[0] // fold
    row = lax.broadcasted_iota(jnp.int32, (rows_l, n_occ), 0)
    col = lax.broadcasted_iota(jnp.int32, (rows_l, n_occ), 1)
    for j in range(fold):
        ctl[j * rows_l:(j + 1) * rows_l, :] = rows_of_ct((row <= pairs * n_orb) & (col == row * fold + j))
    pick = lax.broadcasted_iota(jnp.int32, (row_blk, n_bf), 0)
    pick_col = lax.broadcasted_iota(jnp.int32, (row_blk, n_bf), 1)
    own = mm((pick + me * row_blk == pick_col).astype(jnp.float32), occ_t, 1, 1)
    dens[...] = mm(own, occ_t, 1, 0)

    def t_copy(g, dst, src_dev):
        m0, mg, base = groups[g]
        return pltpu.make_async_remote_copy(
            src_ref=send.at[dst, pl.ds(base, slots * mg)], dst_ref=recv.at[src_dev, pl.ds(base, slots * mg)],
            send_sem=t_ss.at[g, dst], recv_sem=t_rs.at[g, src_dev], device_id={'orb': dst}, device_id_type=MESH_ID)

    def l_copy(dst, src_dev):
        return pltpu.make_async_remote_copy(
            src_ref=ex_send.at[dst], dst_ref=ex_recv.at[src_dev], send_sem=l_ss.at[dst], recv_sem=l_rs.at[src_dev],
            device_id={'orb': dst}, device_id_type=MESH_ID)

    def g_copy(dst, src_dev):
        return pltpu.make_async_remote_copy(
            src_ref=gsend, dst_ref=grecv.at[src_dev], send_sem=g_ss.at[dst], recv_sem=g_rs.at[src_dev],
            device_id={'orb': dst}, device_id_type=MESH_ID)

    def j_copy(dst, src_dev):
        return pltpu.make_async_remote_copy(
            src_ref=jsend.at[dst], dst_ref=jrecv.at[src_dev], send_sem=j_ss.at[dst], recv_sem=j_rs.at[src_dev],
            device_id={'aux': dst}, device_id_type=MESH_ID)

    def k_copy(orb, aux, src_dev):
        slot = aux * n_orb + orb
        return pltpu.make_async_remote_copy(
            src_ref=ksend.at[slot], dst_ref=krecv.at[src_dev], send_sem=k_ss.at[slot], recv_sem=k_rs.at[src_dev],
            device_id={'orb': orb, 'aux': aux}, device_id_type=MESH_ID)

    def ex_row(slot, m, tail):
        return (n_ex * whole + slot * rest + m - whole) if tail else (slot * whole + m)

    n_ex = pairs + 1

    def t_rows(g):
        m0, mg, base = groups[g]
        tail = m0 >= whole
        load_list[g].wait()

        def step(m, carry):
            block = mm(ctp[...], bv[m, 0:q_main, :], 1, 1)
            for d in range(n_orb):
                for t in range(n_tiles):
                    piece = block[d * SUBL:d * SUBL + occ_each, t * LANES:(t + 1) * LANES]
                    send[d, pl.ds(base + t * occ_each * mg + m - m0, occ_each, stride=mg), :] = piece
                    if d // extra == t:
                        at = d * SUBL + occ_each
                        ex_send[d, pl.ds(ex_row(pairs, m, tail), 1), :] = block[at:at + 1, t * LANES:(t + 1) * LANES]
            return carry

        lax.fori_loop(m0, m0 + mg, step, 0)

    def t_send(g):
        for r in ORDER:
            t_copy(g, peer_orb(r), me).start()
        m0, mg, base = groups[g]
        recv[me, base:base + slots * mg, :] = send[me, base:base + slots * mg, :]

    def left_rows():
        for m0, m1 in ((0, whole), (whole, row_blk)):
            tail = m0 >= whole

            def step(m, carry):
                rows = jnp.concatenate([bv[m, q_main:q_loc, :], jnp.zeros((left_pad - q_left, n_bf), jnp.float32)], axis=0)
                block = mm(ctl[...], rows, 1, 1)
                block = jnp.concatenate([block, jnp.zeros((fold * rows_l, LANES - left_pad), jnp.float32)], axis=1)
                total = block[0:rows_l]
                for j in range(1, fold):
                    total = total + pltpu.roll(block[j * rows_l:(j + 1) * rows_l], j * left_pad, 1)
                for d in range(n_orb):
                    for u in range(pairs):
                        ex_send[d, pl.ds(ex_row(u, m, tail), 1), :] = total[d * pairs + u:d * pairs + u + 1]
                d = n_tiles * extra
                ex_send[d, pl.ds(ex_row(pairs, m, tail), 1), :] = total[n_orb * pairs:n_orb * pairs + 1]
                return carry

            lax.fori_loop(m0, m1, step, 0)

    def gamma_part():
        q_step = 5 * SUBL
        for q0 in range(0, q_loc, q_step):
            n_q = min(q_step, q_loc - q0)

            def body(m, acc):
                return acc + bv[m, q0:q0 + n_q, :] * dens[pl.ds(m, 1), :]

            srow[q0:q0 + n_q, :] = lax.fori_loop(0, row_blk, body, jnp.zeros((n_q, n_bf), jnp.float32), unroll=3)
        total = jnp.zeros(gsend.shape, jnp.float32)
        for k in range(srow.shape[0] // LANES):
            row_k = (lax.broadcasted_iota(jnp.int32, (gsend.shape[0], n_bf), 0) == k).astype(jnp.float32)
            total = total + mm(row_k, srow[k * LANES:(k + 1) * LANES, :], 1, 1)
        gsend[...] = total
        grecv[me] = total
        for r in ORDER:
            g_copy(peer_orb(r), me).start()

    def coulomb():
        for r in range(1, n_orb):
            g_copy(me, peer_orb(r)).wait_recv()
        gam = grecv[0]
        for src in range(1, n_orb):
            gam = gam + grecv[src]
        for k in range(srow.shape[0] // LANES):
            row_k = (lax.broadcasted_iota(jnp.int32, (gsend.shape[0], n_bf), 0) == k).astype(jnp.float32)
            gbc[k * LANES:(k + 1) * LANES, :] = mm(gam, row_k, 0, 0)

        def body(m, carry):
            jrows[pl.ds(m, 1), 0:n_bf] = jnp.sum(bv[m] * gbc[0:q_loc, :], axis=0, keepdims=True)
            return carry

        lax.fori_loop(0, row_blk, body, 0)
        jpad = jrows[...]
        for a in range(n_aux):
            piece = jpad if a == 0 else pltpu.roll(jpad, 2 * LANES - a * n_cols, 1)
            jsend[a] = piece[:, 0:LANES]
        jrecv[my] = jsend[my]
        for r in range(1, n_aux):
            j_copy(lax.rem(my + r, n_aux), my).start()

    def collect(g):
        m0, mg, base = groups[g]
        for r in range(1, n_orb):
            t_copy(g, me, peer_orb(r)).wait_recv()
        for src in range(n_orb):
            for s in range(slots):
                xa[src * row_pad + m0:src * row_pad + m0 + mg, s * LANES:(s + 1) * LANES] = recv[src, base + s * mg:base + (s + 1) * mg, :]

    def collect_left():
        for r in range(1, n_orb):
            l_copy(me, peer_orb(r)).wait_recv()
        for src in range(n_orb):
            for s in range(n_ex):
                cols = slice((slots + s) * LANES, (slots + s + 1) * LANES)
                xa[src * row_pad:src * row_pad + whole, cols] = ex_recv[src, s * whole:(s + 1) * whole, :]
                at = n_ex * whole + s * rest
                xa[src * row_pad + whole:src * row_pad + row_blk, cols] = ex_recv[src, at:at + rest, :]

    for g in range(3):
        t_rows(g)
        if g == 0:
            pl.semaphore_wait(barrier, n_dev - 1)
        t_send(g)
    for g in range(3, n_groups):
        load_list[g].wait()
    load_list = load_list[:3] + [Loaded()] * (n_groups - 3)
    gamma_part()
    for g in range(3, n_groups):
        t_rows(g)
        t_send(g)
    left_rows()
    for r in ORDER:
        l_copy(peer_orb(r), me).start()
    ex_recv[me] = ex_send[me]
    xa[...] = jnp.zeros(xa.shape, jnp.float32)
    coulomb()
    for g in range(n_groups):
        collect(g)
    step_k = 4 * LANES
    kacc[...] = mm(xa[:, 0:step_k], xa[:, 0:step_k], 1, 1)
    for c0 in range(step_k, slots * LANES, step_k):
        part = xa[:, c0:c0 + step_k]
        kacc[...] += mm(part, part, 1, 1)
    collect_left()
    part = xa[:, slots * LANES:]
    kacc[...] += mm(part, part, 1, 1)

    half = row_pad // 2
    low_half = lax.broadcasted_iota(jnp.int32, (half, LANES), 1) < LANES // 2
    for orb in range(n_orb):
        for ctile in range(n_aux // 2):
            blk = kacc[orb * row_pad:(orb + 1) * row_pad, ctile * LANES:(ctile + 1) * LANES]
            top, bot = blk[0:half], blk[half:]
            ksend[2 * ctile * n_orb + orb] = jnp.where(low_half, top, pltpu.roll(bot, LANES // 2, 1))
            ksend[(2 * ctile + 1) * n_orb + orb] = jnp.where(low_half, pltpu.roll(top, LANES // 2, 1), bot)
    dev = my * n_orb + me
    krecv[dev] = ksend[dev]

    def k_send(step, carry):
        k_copy(lax.rem(me + lax.rem(step, n_orb), n_orb), lax.rem(my + step // n_orb, n_aux), dev).start()
        return carry

    lax.fori_loop(1, n_dev, k_send, 0)
    for r in range(1, n_aux):
        j_copy(my, lax.rem(my + r, n_aux)).wait_recv()
    jsum = jrecv[0]
    for src in range(1, n_aux):
        jsum = jsum + jrecv[src]

    def k_wait(step, carry):
        src = lax.rem(my + step // n_orb, n_aux) * n_orb + lax.rem(me + lax.rem(step, n_orb), n_orb)
        k_copy(me, my, src).wait_recv()
        return carry

    lax.fori_loop(1, n_dev, k_wait, 0)
    ksum = krecv[0]
    for src in range(1, n_dev):
        ksum = ksum + krecv[src]
    kblk = jnp.concatenate([ksum, pltpu.roll(ksum, LANES // 2, 1)], axis=0)
    pad_cols = row_pad - row_blk
    kcols = jnp.where(lax.broadcasted_iota(jnp.int32, (row_pad, LANES), 1) < row_blk, kblk, pltpu.roll(kblk, LANES - pad_cols, 1))
    out = 2.0 * jsum - kcols
    out_ref[...] = out[0:row_blk, 0:n_cols]

    for g in range(n_groups):
        for r in range(1, n_orb):
            t_copy(g, peer_orb(r), me).wait_send()
    for r in range(1, n_orb):
        l_copy(peer_orb(r), me).wait_send()
        g_copy(peer_orb(r), me).wait_send()
    for r in range(1, n_aux):
        j_copy(lax.rem(my + r, n_aux), my).wait_send()

    def k_drain(step, carry):
        k_copy(lax.rem(me + lax.rem(step, n_orb), n_orb), lax.rem(my + step // n_orb, n_aux), dev).wait_send()
        return carry

    lax.fori_loop(1, n_dev, k_drain, 0)


def solution(mesh):
    n_orb = mesh.shape['orb']
    n_aux = mesh.shape['aux']

    def local_fock(fit_loc, orbitals):
        q_loc, row_blk, n_bf = fit_loc.shape
        n_occ = orbitals.shape[1]
        n_cols = n_bf // n_aux
        row_pad = rup(row_blk, SUBL)
        occ_each = n_occ // n_orb
        q_main = q_loc // LANES * LANES
        n_tiles = q_main // LANES
        slots = n_tiles * occ_each
        whole = row_blk // SUBL * SUBL
        left_pad = rup(q_loc - q_main, SUBL)
        fold = LANES // left_pad
        pairs = occ_each // fold
        n_ex = pairs + 1
        extra = n_occ - n_orb * occ_each
        groups, base = [], 0
        for m0, mg in ((whole, 2), (whole + 2, row_blk - whole - 2)) + tuple((m0, SUBL) for m0 in range(0, whole, SUBL)):
            groups.append((m0, mg, base))
            base += slots * mg
            assert slots * mg % SUBL == 0
        assert n_orb == 2 * n_aux and n_cols == 2 * row_blk and occ_each % fold == 0 and occ_each < SUBL
        assert 0 < extra <= fold and (n_tiles + 1) * extra <= n_orb + 1 and row_pad * n_orb == 2 * LANES
        dims = (n_orb, n_aux, q_loc, row_blk, n_bf, n_occ, row_pad, occ_each, tuple(groups), q_main, left_pad, fold, n_cols)
        n_dev = n_orb * n_aux
        n_groups = len(groups)
        ex_rows = n_ex * whole + rup(n_ex * (row_blk - whole), SUBL)
        q_lanes = rup(q_loc, LANES)
        f32 = jnp.float32
        dma = pltpu.SemaphoreType.DMA
        scratch = [
            pltpu.VMEM((row_blk, q_loc, n_bf), f32),
            pltpu.VMEM((n_occ, n_bf), f32),
            pltpu.VMEM((n_orb * SUBL, n_bf), f32),
            pltpu.VMEM((fold * rup(pairs * n_orb + 1, SUBL), n_bf), f32),
            pltpu.VMEM((row_blk, n_bf), f32),
            pltpu.VMEM((n_orb, base, LANES), f32),
            pltpu.VMEM((n_orb, base, LANES), f32),
            pltpu.VMEM((n_orb, ex_rows, LANES), f32),
            pltpu.VMEM((n_orb, ex_rows, LANES), f32),
            pltpu.VMEM((n_orb * row_pad, (slots + n_ex) * LANES), f32),
            pltpu.VMEM((n_orb * row_pad, n_orb * row_pad), f32),
            pltpu.VMEM((q_lanes, n_bf), f32),
            pltpu.VMEM((SUBL, LANES), f32),
            pltpu.VMEM((n_orb, SUBL, LANES), f32),
            pltpu.VMEM((q_lanes, n_bf), f32),
            pltpu.VMEM((row_pad, 2 * LANES), f32),
            pltpu.VMEM((n_aux, row_pad, LANES), f32),
            pltpu.VMEM((n_aux, row_pad, LANES), f32),
            pltpu.VMEM((n_dev, row_pad // 2, LANES), f32),
            pltpu.VMEM((n_dev, row_pad // 2, LANES), f32),
            dma((n_groups + 1,)), dma((n_groups, n_orb)), dma((n_groups, n_orb)), dma((n_orb,)), dma((n_orb,)),
            dma((n_orb,)), dma((n_orb,)), dma((n_aux,)), dma((n_aux,)), dma((n_dev,)), dma((n_dev,)),
        ]
        return pl.pallas_call(
            functools.partial(fock_kernel, dims),
            out_shape=jax.ShapeDtypeStruct((row_blk, n_cols), f32),
            in_specs=[pl.BlockSpec(memory_space=pl.ANY), pl.BlockSpec(memory_space=pl.ANY)],
            out_specs=pl.BlockSpec(memory_space=pltpu.VMEM),
            scratch_shapes=scratch,
            compiler_params=pltpu.CompilerParams(collective_id=0, has_side_effects=True, vmem_limit_bytes=56 * 1024 * 1024),
            name='fock_build',
        )(jnp.transpose(fit_loc, (1, 0, 2)), orbitals.T)

    spec_fit = P(('sys', 'aux'), 'orb', None)
    spec_orbitals = P('sys', None)
    spec_out = P(('sys', 'orb'), 'aux')
    return jax.shard_map(local_fock, mesh=mesh, in_specs=(spec_fit, spec_orbitals), out_specs=spec_out, check_vma=False)
```

```python
import functools
import jax
import jax.numpy as jnp
from jax import lax
from jax.experimental import pallas as pl
from jax.experimental.pallas import tpu as pltpu
from jax.sharding import PartitionSpec as P

PREC_MODE = lax.Precision.HIGHEST
MESH_ID = pl.DeviceIdType.MESH
LANES = 128
SUBL = 8


ORDER = (4, 2, 6, 5, 3, 7, 1)
T_STEP = 2


def mm(lhs, rhs, lhs_dim, rhs_dim):
    return lax.dot_general(lhs, rhs, (((lhs_dim,), (rhs_dim,)), ((), ())), precision=PREC_MODE, preferred_element_type=jnp.float32)


def rup(value, unit):
    return -(-value // unit) * unit


class Loaded:
    def wait(self):
        pass


def fock_kernel(dims, fit_ref, occ_ref, out_ref, bv, ct, ctn, dens, recv, send, ex_recv, ex_send, xa, kacc,
                srow, gsend, grecv, gbc, jrows, jsend, jrecv, ksend, krecv,
                load_sem, t_ss, t_rs, l_ss, l_rs, g_ss, g_rs, j_ss, j_rs, k_ss, k_rs):
    (n_orb, n_aux, q_loc, row_blk, n_bf, n_occ, row_pad, occ_each, groups, q_main, left_pad, fold, n_cols) = dims
    me = lax.axis_index('orb')
    my = lax.axis_index('aux')
    n_dev = n_orb * n_aux
    n_tiles = q_main // LANES
    slots = n_tiles * occ_each
    n_groups = len(groups)
    q_left = q_loc - q_main
    whole = row_blk // SUBL * SUBL
    rest = row_blk - whole
    pairs = occ_each // fold
    extra = n_occ - n_orb * occ_each

    def peer_orb(step):
        return lax.rem(me + step, n_orb)

    occ_load = pltpu.make_async_copy(occ_ref, ct, load_sem.at[n_groups])
    occ_load.start()
    load_list = [pltpu.make_async_copy(fit_ref.at[pl.ds(m0, mg)], bv.at[pl.ds(m0, mg)], load_sem.at[g]) for g, (m0, mg, base) in enumerate(groups)]
    for cp in load_list:
        cp.start()

    barrier = pltpu.get_barrier_semaphore()

    for r in range(1, n_orb):
        pl.semaphore_signal(barrier, inc=1, device_id={'orb': peer_orb(r)}, device_id_type=MESH_ID)
    for r in range(1, n_aux):
        pl.semaphore_signal(barrier, inc=1, device_id={'aux': lax.rem(my + r, n_aux)}, device_id_type=MESH_ID)
    ex_send[...] = jnp.zeros(ex_send.shape, jnp.float32)

    occ_load.wait()
    occ_t = ct[...]
    rows_l = rup(pairs * n_orb + 1, SUBL)
    row = lax.broadcasted_iota(jnp.int32, (n_occ, LANES), 0)
    col = lax.broadcasted_iota(jnp.int32, (n_occ, LANES), 1)
    in_blk = col % SUBL
    which = (((in_blk < occ_each) & (row == col // SUBL * occ_each + in_blk))
             | ((in_blk == occ_each) & (row == n_orb * occ_each + col // SUBL % extra))) & (col < n_orb * SUBL)
    ctn[:, 0:LANES] = mm(occ_t, which.astype(jnp.float32), 0, 0)
    in_blk = col % rows_l
    which = (in_blk <= pairs * n_orb) & (row == in_blk * fold + col // rows_l) & (col < fold * rows_l)
    ctn[:, LANES:] = mm(occ_t, which.astype(jnp.float32), 0, 0)
    pick = lax.broadcasted_iota(jnp.int32, (row_blk, n_bf), 0)
    pick_col = lax.broadcasted_iota(jnp.int32, (row_blk, n_bf), 1)
    own = mm((pick + me * row_blk == pick_col).astype(jnp.float32), occ_t, 1, 1)
    dens[...] = mm(own, occ_t, 1, 0)

    def t_copy(g, dst, src_dev):
        m0, mg, base = groups[g]
        return pltpu.make_async_remote_copy(
            src_ref=send.at[dst, pl.ds(base, slots * mg)], dst_ref=recv.at[src_dev, pl.ds(base, slots * mg)],
            send_sem=t_ss.at[g, dst], recv_sem=t_rs.at[g, src_dev], device_id={'orb': dst}, device_id_type=MESH_ID)

    def l_copy(dst, src_dev):
        return pltpu.make_async_remote_copy(
            src_ref=ex_send.at[dst], dst_ref=ex_recv.at[src_dev], send_sem=l_ss.at[dst], recv_sem=l_rs.at[src_dev],
            device_id={'orb': dst}, device_id_type=MESH_ID)

    def g_copy(dst, src_dev):
        return pltpu.make_async_remote_copy(
            src_ref=gsend, dst_ref=grecv.at[src_dev], send_sem=g_ss.at[dst], recv_sem=g_rs.at[src_dev],
            device_id={'orb': dst}, device_id_type=MESH_ID)

    def j_copy(dst, src_dev):
        return pltpu.make_async_remote_copy(
            src_ref=jsend.at[dst], dst_ref=jrecv.at[src_dev], send_sem=j_ss.at[dst], recv_sem=j_rs.at[src_dev],
            device_id={'aux': dst}, device_id_type=MESH_ID)

    def k_copy(orb, aux, src_dev):
        slot = aux * n_orb + orb
        return pltpu.make_async_remote_copy(
            src_ref=ksend.at[slot], dst_ref=krecv.at[src_dev], send_sem=k_ss.at[slot], recv_sem=k_rs.at[src_dev],
            device_id={'orb': orb, 'aux': aux}, device_id_type=MESH_ID)

    def ex_row(slot, m, tail):
        return (n_ex * whole + slot * rest + m - whole) if tail else (slot * whole + m)

    n_ex = pairs + 1

    def t_rows(g):
        m0, mg, base = groups[g]
        tail = m0 >= whole
        load_list[g].wait()

        def rows_of(m):
            return [bv[m, 0:q_main, :], bv[m, q_main:q_loc, :], jnp.zeros((left_pad - q_left, n_bf), jnp.float32)]

        def put(m, block, left):
            for d in range(n_orb):
                for t in range(n_tiles):
                    piece = block[d * SUBL:d * SUBL + occ_each, t * LANES:(t + 1) * LANES]
                    send[d, pl.ds(base + t * occ_each * mg + m - m0, occ_each, stride=mg), :] = piece
                    if d // extra == t:
                        at = d * SUBL + occ_each
                        ex_send[d, pl.ds(ex_row(pairs, m, tail), 1), :] = block[at:at + 1, t * LANES:(t + 1) * LANES]
            total = left[0:rows_l]
            for j in range(1, fold):
                total = total + pltpu.roll(left[j * rows_l:(j + 1) * rows_l], j * left_pad, 1)
            for d in range(n_orb):
                for u in range(pairs):
                    ex_send[d, pl.ds(ex_row(u, m, tail), 1), :] = total[d * pairs + u:d * pairs + u + 1]
            d = n_tiles * extra
            ex_send[d, pl.ds(ex_row(pairs, m, tail), 1), :] = total[n_orb * pairs:n_orb * pairs + 1]

        def step(k, carry):
            m = m0 + k * T_STEP
            rows = jnp.concatenate(sum([rows_of(m + j) for j in range(T_STEP)], []), axis=0)
            block = mm(rows, ctn[...], 1, 0)
            for j in range(T_STEP):
                at = j * (q_main + left_pad)
                left = block[at + q_main:at + q_main + left_pad, LANES:]
                left = jnp.concatenate([left, jnp.zeros((LANES - left_pad, LANES), jnp.float32)], axis=0)
                put(m + j, block[at:at + q_main, 0:LANES].T, left.T)
            return carry

        lax.fori_loop(0, mg // T_STEP, step, 0)

    def t_send(g):
        for r in ORDER:
            t_copy(g, peer_orb(r), me).start()
        m0, mg, base = groups[g]
        recv[me, base:base + slots * mg, :] = send[me, base:base + slots * mg, :]

    def gamma_part():
        q_step = 5 * SUBL
        for q0 in range(0, q_loc, q_step):
            n_q = min(q_step, q_loc - q0)

            def body(m, acc):
                return acc + bv[m, q0:q0 + n_q, :] * dens[pl.ds(m, 1), :]

            srow[q0:q0 + n_q, :] = lax.fori_loop(0, row_blk, body, jnp.zeros((n_q, n_bf), jnp.float32), unroll=3)
        total = jnp.zeros(gsend.shape, jnp.float32)
        for k in range(srow.shape[0] // LANES):
            row_k = (lax.broadcasted_iota(jnp.int32, (gsend.shape[0], n_bf), 0) == k).astype(jnp.float32)
            total = total + mm(row_k, srow[k * LANES:(k + 1) * LANES, :], 1, 1)
        gsend[...] = total
        grecv[me] = total
        for r in ORDER:
            g_copy(peer_orb(r), me).start()

    def coulomb():
        for r in range(1, n_orb):
            g_copy(me, peer_orb(r)).wait_recv()
        gam = grecv[0]
        for src in range(1, n_orb):
            gam = gam + grecv[src]
        for k in range(srow.shape[0] // LANES):
            row_k = (lax.broadcasted_iota(jnp.int32, (gsend.shape[0], n_bf), 0) == k).astype(jnp.float32)
            gbc[k * LANES:(k + 1) * LANES, :] = mm(gam, row_k, 0, 0)

        def body(m, carry):
            jrows[pl.ds(m, 1), 0:n_bf] = jnp.sum(bv[m] * gbc[0:q_loc, :], axis=0, keepdims=True)
            return carry

        lax.fori_loop(0, row_blk, body, 0)
        jpad = jrows[...]
        for a in range(n_aux):
            piece = jpad if a == 0 else pltpu.roll(jpad, 2 * LANES - a * n_cols, 1)
            jsend[a] = piece[:, 0:LANES]
        jrecv[my] = jsend[my]
        for r in range(1, n_aux):
            j_copy(lax.rem(my + r, n_aux), my).start()

    def collect(g):
        m0, mg, base = groups[g]
        for r in range(1, n_orb):
            t_copy(g, me, peer_orb(r)).wait_recv()
        for src in range(n_orb):
            for s in range(slots):
                xa[src * row_pad + m0:src * row_pad + m0 + mg, s * LANES:(s + 1) * LANES] = recv[src, base + s * mg:base + (s + 1) * mg, :]

    def collect_left():
        for r in range(1, n_orb):
            l_copy(me, peer_orb(r)).wait_recv()
        for src in range(n_orb):
            for s in range(n_ex):
                cols = slice((slots + s) * LANES, (slots + s + 1) * LANES)
                xa[src * row_pad:src * row_pad + whole, cols] = ex_recv[src, s * whole:(s + 1) * whole, :]
                at = n_ex * whole + s * rest
                xa[src * row_pad + whole:src * row_pad + row_blk, cols] = ex_recv[src, at:at + rest, :]

    t_rows(0)
    t_rows(1)
    pl.semaphore_wait(barrier, n_orb - 1 + n_aux - 1)
    t_send(0)
    t_send(1)
    t_rows(2)
    t_send(2)
    for g in range(3, n_groups):
        load_list[g].wait()
    load_list = load_list[:3] + [Loaded()] * (n_groups - 3)
    gamma_part()
    for g in range(3, n_groups):
        t_rows(g)
        t_send(g)
    for r in ORDER:
        l_copy(peer_orb(r), me).start()
    ex_recv[me] = ex_send[me]
    xa[...] = jnp.zeros(xa.shape, jnp.float32)
    coulomb()
    for g in range(n_groups):
        collect(g)
    step_k = 4 * LANES
    kacc[...] = mm(xa[:, 0:step_k], xa[:, 0:step_k], 1, 1)
    for c0 in range(step_k, slots * LANES, step_k):
        part = xa[:, c0:c0 + step_k]
        kacc[...] += mm(part, part, 1, 1)
    collect_left()
    part = xa[:, slots * LANES:]
    kacc[...] += mm(part, part, 1, 1)

    half = row_pad // 2
    low_half = lax.broadcasted_iota(jnp.int32, (half, LANES), 1) < LANES // 2
    for orb in range(n_orb):
        for ctile in range(n_aux // 2):
            blk = kacc[orb * row_pad:(orb + 1) * row_pad, ctile * LANES:(ctile + 1) * LANES]
            top, bot = blk[0:half], blk[half:]
            ksend[2 * ctile * n_orb + orb] = jnp.where(low_half, top, pltpu.roll(bot, LANES // 2, 1))
            ksend[(2 * ctile + 1) * n_orb + orb] = jnp.where(low_half, pltpu.roll(top, LANES // 2, 1), bot)
    dev = my * n_orb + me
    krecv[dev] = ksend[dev]

    def hops(step, ring):
        return min(step, ring - step)

    steps = sorted(range(1, n_dev), key=lambda k: -(hops((k % n_orb + 1) // 2, n_orb // 2) + hops(k // n_orb, n_aux)))

    def k_out(step):
        return k_copy(peer_orb(step % n_orb), lax.rem(my + step // n_orb, n_aux), dev)

    for step in steps:
        k_out(step).start()
    for r in range(1, n_aux):
        j_copy(my, lax.rem(my + r, n_aux)).wait_recv()
    jsum = jrecv[0]
    for src in range(1, n_aux):
        jsum = jsum + jrecv[src]

    for step in reversed(steps):
        k_copy(me, my, lax.rem(my + step // n_orb, n_aux) * n_orb + peer_orb(step % n_orb)).wait_recv()
    ksum = krecv[0]
    for src in range(1, n_dev):
        ksum = ksum + krecv[src]
    kblk = jnp.concatenate([ksum, pltpu.roll(ksum, LANES // 2, 1)], axis=0)
    pad_cols = row_pad - row_blk
    kcols = jnp.where(lax.broadcasted_iota(jnp.int32, (row_pad, LANES), 1) < row_blk, kblk, pltpu.roll(kblk, LANES - pad_cols, 1))
    out = 2.0 * jsum - kcols
    out_ref[...] = out[0:row_blk, 0:n_cols]

    for g in range(n_groups):
        for r in range(1, n_orb):
            t_copy(g, peer_orb(r), me).wait_send()
    for r in range(1, n_orb):
        l_copy(peer_orb(r), me).wait_send()
        g_copy(peer_orb(r), me).wait_send()
    for r in range(1, n_aux):
        j_copy(lax.rem(my + r, n_aux), my).wait_send()

    for step in steps:
        k_out(step).wait_send()


def solution(mesh):
    n_orb = mesh.shape['orb']
    n_aux = mesh.shape['aux']

    def local_fock(fit_loc, orbitals):
        q_loc, row_blk, n_bf = fit_loc.shape
        n_occ = orbitals.shape[1]
        n_cols = n_bf // n_aux
        row_pad = rup(row_blk, SUBL)
        occ_each = n_occ // n_orb
        q_main = q_loc // LANES * LANES
        n_tiles = q_main // LANES
        slots = n_tiles * occ_each
        whole = row_blk // SUBL * SUBL
        left_pad = rup(q_loc - q_main, SUBL)
        fold = LANES // left_pad
        pairs = occ_each // fold
        n_ex = pairs + 1
        extra = n_occ - n_orb * occ_each
        groups, base = [], 0
        for m0, mg in ((whole, 2), (whole + 2, row_blk - whole - 2)) + tuple((m0, SUBL) for m0 in range(0, whole, SUBL)):
            groups.append((m0, mg, base))
            base += slots * mg
            assert slots * mg % SUBL == 0
        assert n_orb == 2 * n_aux and n_cols == 2 * row_blk and occ_each % fold == 0 and occ_each < SUBL
        assert 0 < extra <= fold and (n_tiles + 1) * extra <= n_orb + 1 and row_pad * n_orb == 2 * LANES
        dims = (n_orb, n_aux, q_loc, row_blk, n_bf, n_occ, row_pad, occ_each, tuple(groups), q_main, left_pad, fold, n_cols)
        n_dev = n_orb * n_aux
        n_groups = len(groups)
        ex_rows = n_ex * whole + rup(n_ex * (row_blk - whole), SUBL)
        q_lanes = rup(q_loc, LANES)
        f32 = jnp.float32
        dma = pltpu.SemaphoreType.DMA
        scratch = [
            pltpu.VMEM((row_blk, q_loc, n_bf), f32),
            pltpu.VMEM((n_occ, n_bf), f32),
            pltpu.VMEM((n_bf, 2 * LANES), f32),
            pltpu.VMEM((row_blk, n_bf), f32),
            pltpu.VMEM((n_orb, base, LANES), f32),
            pltpu.VMEM((n_orb, base, LANES), f32),
            pltpu.VMEM((n_orb, ex_rows, LANES), f32),
            pltpu.VMEM((n_orb, ex_rows, LANES), f32),
            pltpu.VMEM((n_orb * row_pad, (slots + n_ex) * LANES), f32),
            pltpu.VMEM((n_orb * row_pad, n_orb * row_pad), f32),
            pltpu.VMEM((q_lanes, n_bf), f32),
            pltpu.VMEM((SUBL, LANES), f32),
            pltpu.VMEM((n_orb, SUBL, LANES), f32),
            pltpu.VMEM((q_lanes, n_bf), f32),
            pltpu.VMEM((row_pad, 2 * LANES), f32),
            pltpu.VMEM((n_aux, row_pad, LANES), f32),
            pltpu.VMEM((n_aux, row_pad, LANES), f32),
            pltpu.VMEM((n_dev, row_pad // 2, LANES), f32),
            pltpu.VMEM((n_dev, row_pad // 2, LANES), f32),
            dma((n_groups + 1,)), dma((n_groups, n_orb)), dma((n_groups, n_orb)), dma((n_orb,)), dma((n_orb,)),
            dma((n_orb,)), dma((n_orb,)), dma((n_aux,)), dma((n_aux,)), dma((n_dev,)), dma((n_dev,)),
        ]
        return pl.pallas_call(
            functools.partial(fock_kernel, dims),
            out_shape=jax.ShapeDtypeStruct((row_blk, n_cols), f32),
            in_specs=[pl.BlockSpec(memory_space=pl.ANY), pl.BlockSpec(memory_space=pl.ANY)],
            out_specs=pl.BlockSpec(memory_space=pltpu.VMEM),
            scratch_shapes=scratch,
            compiler_params=pltpu.CompilerParams(collective_id=0, has_side_effects=True, vmem_limit_bytes=56 * 1024 * 1024),
            name='fock_build',
        )(jnp.transpose(fit_loc, (1, 0, 2)), orbitals.T)

    spec_fit = P(('sys', 'aux'), 'orb', None)
    spec_orbitals = P('sys', None)
    spec_out = P(('sys', 'orb'), 'aux')
    return jax.shard_map(local_fock, mesh=mesh, in_specs=(spec_fit, spec_orbitals), out_specs=spec_out, check_vma=False)
```

```python
import functools
import jax
import jax.numpy as jnp
from jax import lax
from jax.experimental import pallas as pl
from jax.experimental.pallas import tpu as pltpu
from jax.sharding import PartitionSpec as P

PREC_MODE = lax.Precision.HIGHEST
MESH_ID = pl.DeviceIdType.MESH
LANES = 128
SUBL = 8


ORDER = (4, 2, 6, 5, 3, 7, 1)
SMALL_STEP = 6
WHOLE_STEP = 8


def mm(lhs, rhs, lhs_dim, rhs_dim):
    return lax.dot_general(lhs, rhs, (((lhs_dim,), (rhs_dim,)), ((), ())), precision=PREC_MODE, preferred_element_type=jnp.float32)


def rup(value, unit):
    return -(-value // unit) * unit


def fock_kernel(dims, fit_ref, occ_ref, out_ref, bv, ct, ctn, dens, recv, send, ex_recv, ex_send, xa, kacc,
                srow, gsend, grecv, gbc, jrows, jsend, jrecv, ksend, krecv,
                load_sem, t_ss, t_rs, l_ss, l_rs, g_ss, g_rs, j_ss, j_rs, k_ss, k_rs):
    (n_orb, n_aux, q_loc, row_blk, n_bf, n_occ, row_pad, occ_each, q_main, left_pad, fold, n_cols) = dims
    me = lax.axis_index('orb')
    my = lax.axis_index('aux')
    n_dev = n_orb * n_aux
    n_tiles = q_main // LANES
    slots = n_tiles * occ_each
    q_left = q_loc - q_main
    whole = row_blk // SUBL * SUBL
    rest = row_blk - whole
    pairs = occ_each // fold
    extra = n_occ - n_orb * occ_each

    def peer_orb(step):
        return lax.rem(me + step, n_orb)

    n_small = 1
    n_whole = whole // SUBL
    n_groups = n_small + n_whole
    small_rows, whole_rows = slots * rest, slots * SUBL

    def load(first, count, sem):
        return pltpu.make_async_copy(fit_ref.at[pl.ds(first, count)], bv.at[pl.ds(first, count)], load_sem.at[sem])

    def small_load(k):
        return load(whole, rest, k)

    def whole_load(k):
        return load(k * SUBL, SUBL, n_small + k)

    occ_load = pltpu.make_async_copy(occ_ref, ct, load_sem.at[n_groups])
    occ_load.start()
    for k in range(n_small):
        small_load(k).start()
    for k in range(n_whole):
        whole_load(k).start()

    barrier = pltpu.get_barrier_semaphore()

    for r in range(1, n_orb):
        pl.semaphore_signal(barrier, inc=1, device_id={'orb': peer_orb(r)}, device_id_type=MESH_ID)
    for r in range(1, n_aux):
        pl.semaphore_signal(barrier, inc=1, device_id={'aux': lax.rem(my + r, n_aux)}, device_id_type=MESH_ID)
    ex_send[...] = jnp.zeros(ex_send.shape, jnp.float32)

    occ_load.wait()
    occ_t = ct[...]
    rows_l = rup(pairs * n_orb + 1, SUBL)
    row = lax.broadcasted_iota(jnp.int32, (n_occ, LANES), 0)
    col = lax.broadcasted_iota(jnp.int32, (n_occ, LANES), 1)
    in_blk = col % SUBL
    which = (((in_blk < occ_each) & (row == col // SUBL * occ_each + in_blk))
             | ((in_blk == occ_each) & (row == n_orb * occ_each + col // SUBL % extra))) & (col < n_orb * SUBL)
    ctn[:, 0:LANES] = mm(occ_t, which.astype(jnp.float32), 0, 0)
    in_blk = col % rows_l
    which = (in_blk <= pairs * n_orb) & (row == in_blk * fold + col // rows_l) & (col < fold * rows_l)
    ctn[:, LANES:] = mm(occ_t, which.astype(jnp.float32), 0, 0)
    def t_copy(is_small, k, dst, src_dev):
        rows = pl.ds(pl.multiple_of(k * small_rows, SUBL), small_rows) if is_small else pl.ds(pl.multiple_of(n_small * small_rows + k * whole_rows, SUBL), whole_rows)
        g = k if is_small else n_small + k
        return pltpu.make_async_remote_copy(
            src_ref=send.at[dst, rows], dst_ref=recv.at[src_dev, rows],
            send_sem=t_ss.at[g, dst], recv_sem=t_rs.at[g, src_dev], device_id={'orb': dst}, device_id_type=MESH_ID)

    t_groups = [(True, k) for k in range(n_small)] + [(False, k) for k in range(n_whole)]

    def l_copy(part, dst, src_dev):
        rows = pl.ds(0, last_row) if part == 0 else pl.ds(last_row, ex_send.shape[1] - last_row)
        return pltpu.make_async_remote_copy(
            src_ref=ex_send.at[dst, rows], dst_ref=ex_recv.at[src_dev, rows], send_sem=l_ss.at[part, dst], recv_sem=l_rs.at[part, src_dev],
            device_id={'orb': dst}, device_id_type=MESH_ID)

    def if_last(dst, act):
        pl.when(dst <= n_tiles * extra)(act)

    def g_copy(dst, src_dev):
        return pltpu.make_async_remote_copy(
            src_ref=gsend, dst_ref=grecv.at[src_dev], send_sem=g_ss.at[dst], recv_sem=g_rs.at[src_dev],
            device_id={'orb': dst}, device_id_type=MESH_ID)

    def j_copy(dst, src_dev):
        return pltpu.make_async_remote_copy(
            src_ref=jsend.at[dst], dst_ref=jrecv.at[src_dev], send_sem=j_ss.at[dst], recv_sem=j_rs.at[src_dev],
            device_id={'aux': dst}, device_id_type=MESH_ID)

    def k_copy(orb, aux, src_dev):
        slot = aux * n_orb + orb
        return pltpu.make_async_remote_copy(
            src_ref=ksend.at[slot], dst_ref=krecv.at[src_dev], send_sem=k_ss.at[slot], recv_sem=k_rs.at[src_dev],
            device_id={'orb': orb, 'aux': aux}, device_id_type=MESH_ID)

    def ex_row(slot, m, tail):
        if slot == pairs:
            return last_row + m
        return (pairs * whole + slot * rest + m - whole) if tail else (slot * whole + m)

    last_row = rup(pairs * row_blk, SUBL)

    def t_part(count, m, at, mg, tail):

        def rows_of(m):
            return [bv[m, 0:q_main, :], bv[m, q_main:q_loc, :], jnp.zeros((left_pad - q_left, n_bf), jnp.float32)]

        def put(m, at_m, block, left):
            for d in range(n_orb):
                for t in range(n_tiles):
                    piece = block[d * SUBL:d * SUBL + occ_each, t * LANES:(t + 1) * LANES]
                    send[d, pl.ds(at_m + t * occ_each * mg, occ_each, stride=mg), :] = piece
                    if d // extra == t:
                        pick = d * SUBL + occ_each
                        ex_send[d, pl.ds(ex_row(pairs, m, tail), 1), :] = block[pick:pick + 1, t * LANES:(t + 1) * LANES]
            total = left[0:rows_l]
            for j in range(1, fold):
                total = total + pltpu.roll(left[j * rows_l:(j + 1) * rows_l], j * left_pad, 1)
            for d in range(n_orb):
                for u in range(pairs):
                    ex_send[d, pl.ds(ex_row(u, m, tail), 1), :] = total[d * pairs + u:d * pairs + u + 1]
            d = n_tiles * extra
            ex_send[d, pl.ds(ex_row(pairs, m, tail), 1), :] = total[n_orb * pairs:n_orb * pairs + 1]

        rows = jnp.concatenate(sum([rows_of(m + j) for j in range(count)], []), axis=0)
        block = mm(rows, ctn[...], 1, 0)
        for j in range(count):
            top = j * (q_main + left_pad)
            left = block[top + q_main:top + q_main + left_pad, LANES:]
            left = jnp.concatenate([left, jnp.zeros((LANES - left_pad, LANES), jnp.float32)], axis=0)
            put(m + j, at + j, block[top:top + q_main, 0:LANES].T, left.T)

    def t_send(is_small, k):
        for r in ORDER:
            t_copy(is_small, k, peer_orb(r), me).start()

    def t_small():
        small_load(0).wait()

        def step(j, carry):
            t_part(SMALL_STEP, whole + j * SMALL_STEP, j * SMALL_STEP, rest, True)
            return carry

        lax.fori_loop(0, rest // SMALL_STEP, step, 0)
        pl.semaphore_wait(barrier, n_orb - 1 + n_aux - 1)
        t_send(True, 0)

    def t_whole(k, carry):
        @pl.when(k < n_whole - 1)
        def _():
            whole_load(k).wait()

        def step(j, inner):
            t_part(WHOLE_STEP, k * SUBL + j * WHOLE_STEP, n_small * small_rows + k * whole_rows + j * WHOLE_STEP, SUBL, False)
            return inner

        lax.fori_loop(0, SUBL // WHOLE_STEP, step, 0)
        t_send(False, k)

        @pl.when(k == n_whole - 2)
        def _():
            gamma_part()
        return carry

    def gamma_part():
        whole_load(n_whole - 1).wait()
        pick = lax.broadcasted_iota(jnp.int32, (row_blk, n_bf), 0)
        pick_col = lax.broadcasted_iota(jnp.int32, (row_blk, n_bf), 1)
        own = mm((pick + me * row_blk == pick_col).astype(jnp.float32), occ_t, 1, 1)
        dens[...] = mm(own, occ_t, 1, 0)
        q_step = 5 * SUBL
        for q0 in range(0, q_loc, q_step):
            n_q = min(q_step, q_loc - q0)

            def body(m, acc):
                return acc + bv[m, q0:q0 + n_q, :] * dens[pl.ds(m, 1), :]

            srow[q0:q0 + n_q, :] = lax.fori_loop(0, row_blk, body, jnp.zeros((n_q, n_bf), jnp.float32), unroll=3)
        total = jnp.zeros(gsend.shape, jnp.float32)
        for k in range(srow.shape[0] // LANES):
            row_k = (lax.broadcasted_iota(jnp.int32, (gsend.shape[0], n_bf), 0) == k).astype(jnp.float32)
            total = total + mm(row_k, srow[k * LANES:(k + 1) * LANES, :], 1, 1)
        gsend[...] = total
        grecv[me] = total
        for r in ORDER:
            g_copy(peer_orb(r), me).start()

    def coulomb():
        for r in range(1, n_orb):
            g_copy(me, peer_orb(r)).wait_recv()
        gam = grecv[0]
        for src in range(1, n_orb):
            gam = gam + grecv[src]
        for k in range(srow.shape[0] // LANES):
            row_k = (lax.broadcasted_iota(jnp.int32, (gsend.shape[0], n_bf), 0) == k).astype(jnp.float32)
            gbc[k * LANES:(k + 1) * LANES, :] = mm(gam, row_k, 0, 0)

        def body(m, carry):
            jrows[pl.ds(m, 1), 0:n_bf] = jnp.sum(bv[m] * gbc[0:q_loc, :], axis=0, keepdims=True)
            return carry

        lax.fori_loop(0, row_blk, body, 0)
        jpad = jrows[...]
        for a in range(n_aux):
            piece = jpad if a == 0 else pltpu.roll(jpad, 2 * LANES - a * n_cols, 1)
            jsend[a] = piece[:, 0:LANES]
        jrecv[my] = jsend[my]
        for r in range(1, n_aux):
            j_copy(lax.rem(my + r, n_aux), my).start()

    def collect():
        for is_small, k in t_groups:
            for r in range(1, n_orb):
                t_copy(is_small, k, me, peer_orb(r)).wait_recv()
        recv[me] = send[me]

        def small(src, carry):
            for s in range(slots):
                xa[src, whole:row_blk, s * LANES:(s + 1) * LANES] = recv[src, s * rest:(s + 1) * rest, :]
            return carry

        lax.fori_loop(0, n_orb, small, 0)

        def tiles(n, carry):
            src, k = n // n_whole, lax.rem(n, n_whole)
            for s in range(slots):
                at = pl.multiple_of(n_small * small_rows + k * whole_rows + s * SUBL, SUBL)
                xa[src, pl.ds(pl.multiple_of(k * SUBL, SUBL), SUBL), s * LANES:(s + 1) * LANES] = recv[src, pl.ds(at, SUBL), :]
            return carry

        lax.fori_loop(0, n_orb * n_whole, tiles, 0)

    def collect_left(part):
        for r in range(1, n_orb):
            if part == 0:
                l_copy(0, me, peer_orb(r)).wait_recv()
            else:
                if_last(me, l_copy(1, me, peer_orb(r)).wait_recv)
        for src in range(n_orb):
            for s in range(pairs) if part == 0 else (pairs,):
                cols = slice((slots + s) * LANES, (slots + s + 1) * LANES)
                at = ex_row(s, 0, False)
                xa[src, 0:whole, cols] = ex_recv[src, at:at + whole, :]
                at = ex_row(s, whole, True)
                xa[src, whole:row_blk, cols] = ex_recv[src, at:at + rest, :]

    t_small()
    lax.fori_loop(0, n_whole, t_whole, 0)
    for r in ORDER:
        l_copy(0, peer_orb(r), me).start()
    for r in ORDER:
        if_last(peer_orb(r), l_copy(1, peer_orb(r), me).start)
    ex_recv[me] = ex_send[me]
    xa[...] = jnp.zeros(xa.shape, jnp.float32)
    coulomb()
    collect()
    kacc[...] = jnp.zeros(kacc.shape, jnp.float32)
    depth = 2 * LANES
    n_main = slots * LANES // depth

    def k_step(k, carry):
        @pl.when(k == n_main)
        def _():
            collect_left(0)

        @pl.when(k == n_main + 1)
        def _():
            collect_left(1)

        part = xa[:, :, pl.ds(pl.multiple_of(k * depth, depth), depth)].reshape(n_orb * row_pad, depth)
        kacc[...] += mm(part, part, 1, 1)
        return carry

    lax.fori_loop(0, n_main + 2, k_step, 0)

    half = row_pad // 2
    low_half = lax.broadcasted_iota(jnp.int32, (half, LANES), 1) < LANES // 2
    for orb in range(n_orb):
        for ctile in range(n_aux // 2):
            blk = kacc[orb * row_pad:(orb + 1) * row_pad, ctile * LANES:(ctile + 1) * LANES]
            top, bot = blk[0:half], blk[half:]
            ksend[2 * ctile * n_orb + orb] = jnp.where(low_half, top, pltpu.roll(bot, LANES // 2, 1))
            ksend[(2 * ctile + 1) * n_orb + orb] = jnp.where(low_half, pltpu.roll(top, LANES // 2, 1), bot)
    dev = my * n_orb + me
    krecv[dev] = ksend[dev]

    def hops(step, ring):
        return min(step, ring - step)

    steps = sorted(range(1, n_dev), key=lambda k: -(hops((k % n_orb + 1) // 2, n_orb // 2) + hops(k // n_orb, n_aux)))

    def k_out(step):
        return k_copy(peer_orb(step % n_orb), lax.rem(my + step // n_orb, n_aux), dev)

    for step in steps:
        k_out(step).start()
    for is_small, k in t_groups:
        for r in range(1, n_orb):
            t_copy(is_small, k, peer_orb(r), me).wait_send()
    for r in range(1, n_orb):
        l_copy(0, peer_orb(r), me).wait_send()
        if_last(peer_orb(r), l_copy(1, peer_orb(r), me).wait_send)
        g_copy(peer_orb(r), me).wait_send()
    for r in range(1, n_aux):
        j_copy(lax.rem(my + r, n_aux), my).wait_send()
    for r in range(1, n_aux):
        j_copy(my, lax.rem(my + r, n_aux)).wait_recv()
    jsum = jrecv[0]
    for src in range(1, n_aux):
        jsum = jsum + jrecv[src]

    for step in reversed(steps):
        k_copy(me, my, lax.rem(my + step // n_orb, n_aux) * n_orb + peer_orb(step % n_orb)).wait_recv()
    ksum = krecv[0]
    for src in range(1, n_dev):
        ksum = ksum + krecv[src]
    kblk = jnp.concatenate([ksum, pltpu.roll(ksum, LANES // 2, 1)], axis=0)
    pad_cols = row_pad - row_blk
    kcols = jnp.where(lax.broadcasted_iota(jnp.int32, (row_pad, LANES), 1) < row_blk, kblk, pltpu.roll(kblk, LANES - pad_cols, 1))
    out = 2.0 * jsum - kcols
    out_ref[...] = out[0:row_blk, 0:n_cols]

    for step in steps:
        k_out(step).wait_send()


def solution(mesh):
    n_orb = mesh.shape['orb']
    n_aux = mesh.shape['aux']

    def local_fock(fit_loc, orbitals):
        q_loc, row_blk, n_bf = fit_loc.shape
        n_occ = orbitals.shape[1]
        n_cols = n_bf // n_aux
        row_pad = rup(row_blk, SUBL)
        occ_each = n_occ // n_orb
        q_main = q_loc // LANES * LANES
        n_tiles = q_main // LANES
        slots = n_tiles * occ_each
        whole = row_blk // SUBL * SUBL
        left_pad = rup(q_loc - q_main, SUBL)
        fold = LANES // left_pad
        pairs = occ_each // fold
        extra = n_occ - n_orb * occ_each
        base = slots * row_blk
        rest = row_blk - whole
        assert n_orb == 2 * n_aux and n_cols == 2 * row_blk and occ_each % fold == 0 and occ_each < SUBL
        assert 0 < extra <= fold and (n_tiles + 1) * extra <= n_orb + 1 and row_pad * n_orb == 2 * LANES
        dims = (n_orb, n_aux, q_loc, row_blk, n_bf, n_occ, row_pad, occ_each, q_main, left_pad, fold, n_cols)
        n_dev = n_orb * n_aux
        n_groups = 1 + whole // SUBL
        assert rest % SMALL_STEP == 0 and slots * rest % SUBL == 0 and slots % 2 == 0 and pairs == 2
        ex_rows = rup(pairs * row_blk, SUBL) + rup(row_blk, SUBL)
        q_lanes = rup(q_loc, LANES)
        f32 = jnp.float32
        dma = pltpu.SemaphoreType.DMA
        scratch = [
            pltpu.VMEM((row_blk, q_loc, n_bf), f32),
            pltpu.VMEM((n_occ, n_bf), f32),
            pltpu.VMEM((n_bf, 2 * LANES), f32),
            pltpu.VMEM((row_blk, n_bf), f32),
            pltpu.VMEM((n_orb, base, LANES), f32),
            pltpu.VMEM((n_orb, base, LANES), f32),
            pltpu.VMEM((n_orb, ex_rows, LANES), f32),
            pltpu.VMEM((n_orb, ex_rows, LANES), f32),
            pltpu.VMEM((n_orb, row_pad, (slots + pairs + 2) * LANES), f32),
            pltpu.VMEM((n_orb * row_pad, n_orb * row_pad), f32),
            pltpu.VMEM((q_lanes, n_bf), f32),
            pltpu.VMEM((SUBL, LANES), f32),
            pltpu.VMEM((n_orb, SUBL, LANES), f32),
            pltpu.VMEM((q_lanes, n_bf), f32),
            pltpu.VMEM((row_pad, 2 * LANES), f32),
            pltpu.VMEM((n_aux, row_pad, LANES), f32),
            pltpu.VMEM((n_aux, row_pad, LANES), f32),
            pltpu.VMEM((n_dev, row_pad // 2, LANES), f32),
            pltpu.VMEM((n_dev, row_pad // 2, LANES), f32),
            dma((n_groups + 1,)), dma((n_groups, n_orb)), dma((n_groups, n_orb)), dma((2, n_orb)), dma((2, n_orb)),
            dma((n_orb,)), dma((n_orb,)), dma((n_aux,)), dma((n_aux,)), dma((n_dev,)), dma((n_dev,)),
        ]
        return pl.pallas_call(
            functools.partial(fock_kernel, dims),
            out_shape=jax.ShapeDtypeStruct((row_blk, n_cols), f32),
            in_specs=[pl.BlockSpec(memory_space=pltpu.HBM)] * 2,
            out_specs=pl.BlockSpec(memory_space=pltpu.VMEM),
            scratch_shapes=scratch,
            compiler_params=pltpu.CompilerParams(collective_id=0, has_side_effects=True, vmem_limit_bytes=56 * 1024 * 1024),
            name='fock_build',
        )(jnp.transpose(fit_loc, (1, 0, 2)), orbitals.T)

    spec_fit = P(('sys', 'aux'), 'orb', None)
    spec_orbitals = P('sys', None)
    spec_out = P(('sys', 'orb'), 'aux')
    return jax.shard_map(local_fock, mesh=mesh, in_specs=(spec_fit, spec_orbitals), out_specs=spec_out, check_vma=False)
```

```python
import functools
import jax
import jax.numpy as jnp
from jax import lax
from jax.experimental import pallas as pl
from jax.experimental.pallas import tpu as pltpu
from jax.sharding import PartitionSpec as P

PREC_MODE = lax.Precision.HIGHEST
MESH_ID = pl.DeviceIdType.MESH
LANES = 128
SUBL = 8


ORDER = (4, 2, 6, 5, 3, 7, 1)
SMALL_STEP = 6
WHOLE_STEP = 8


def mm(lhs, rhs, lhs_dim, rhs_dim):
    return lax.dot_general(lhs, rhs, (((lhs_dim,), (rhs_dim,)), ((), ())), precision=PREC_MODE, preferred_element_type=jnp.float32)


def rup(value, unit):
    return -(-value // unit) * unit


def fock_kernel(dims, fit_ref, occ_ref, out_ref, bv, ct, ctn, dens, recv, send, ex_recv, ex_send, xa, kacc,
                srow, gsend, grecv, gbc, jrows, jsend, jrecv, ksend, krecv,
                load_sem, t_ss, t_rs, l_ss, l_rs, g_ss, g_rs, j_ss, j_rs, k_ss, k_rs):
    (n_orb, n_aux, q_loc, row_blk, n_bf, n_occ, row_pad, occ_each, q_main, left_pad, fold, n_cols) = dims
    me = lax.axis_index('orb')
    my = lax.axis_index('aux')
    n_dev = n_orb * n_aux
    n_tiles = q_main // LANES
    slots = n_tiles * occ_each
    q_left = q_loc - q_main
    whole = row_blk // SUBL * SUBL
    rest = row_blk - whole
    pairs = occ_each // fold
    extra = n_occ - n_orb * occ_each

    def peer_orb(step):
        return lax.rem(me + step, n_orb)

    n_small = 1
    n_whole = whole // SUBL
    n_groups = n_small + n_whole
    small_rows, whole_rows = slots * rest, slots * SUBL

    def load(first, count, sem):
        return pltpu.make_async_copy(fit_ref.at[pl.ds(first, count)], bv.at[pl.ds(first, count)], load_sem.at[sem])

    def small_load(k):
        return load(whole, rest, k)

    def whole_load(k):
        return load(k * SUBL, SUBL, n_small + k)

    occ_load = pltpu.make_async_copy(occ_ref, ct, load_sem.at[n_groups])
    occ_load.start()
    for k in range(n_small):
        small_load(k).start()
    for k in range(n_whole):
        whole_load(k).start()

    barrier = pltpu.get_barrier_semaphore()

    for r in range(1, n_orb):
        pl.semaphore_signal(barrier, inc=1, device_id={'orb': peer_orb(r)}, device_id_type=MESH_ID)
    for r in range(1, n_aux):
        pl.semaphore_signal(barrier, inc=1, device_id={'aux': lax.rem(my + r, n_aux)}, device_id_type=MESH_ID)
    ex_send[...] = jnp.zeros(ex_send.shape, jnp.float32)

    occ_load.wait()
    occ_t = ct[...]
    rows_l = rup(pairs * n_orb + 1, SUBL)
    row = lax.broadcasted_iota(jnp.int32, (n_occ, LANES), 0)
    col = lax.broadcasted_iota(jnp.int32, (n_occ, LANES), 1)
    in_blk = col % SUBL
    which = (((in_blk < occ_each) & (row == col // SUBL * occ_each + in_blk))
             | ((in_blk == occ_each) & (row == n_orb * occ_each + col // SUBL % extra))) & (col < n_orb * SUBL)
    ctn[:, 0:LANES] = mm(occ_t, which.astype(jnp.float32), 0, 0)
    in_blk = col % rows_l
    which = (in_blk <= pairs * n_orb) & (row == in_blk * fold + col // rows_l) & (col < fold * rows_l)
    ctn[:, LANES:] = mm(occ_t, which.astype(jnp.float32), 0, 0)
    def t_copy(is_small, k, dst, src_dev):
        rows = pl.ds(pl.multiple_of(k * small_rows, SUBL), small_rows) if is_small else pl.ds(pl.multiple_of(n_small * small_rows + k * whole_rows, SUBL), whole_rows)
        g = k if is_small else n_small + k
        return pltpu.make_async_remote_copy(
            src_ref=send.at[dst, rows], dst_ref=recv.at[src_dev, rows],
            send_sem=t_ss.at[g, dst], recv_sem=t_rs.at[g, src_dev], device_id={'orb': dst}, device_id_type=MESH_ID)

    t_groups = [(True, k) for k in range(n_small)] + [(False, k) for k in range(n_whole)]

    def l_copy(part, dst, src_dev):
        rows = pl.ds(0, last_row) if part == 0 else pl.ds(last_row, ex_send.shape[1] - last_row)
        return pltpu.make_async_remote_copy(
            src_ref=ex_send.at[dst, rows], dst_ref=ex_recv.at[src_dev, rows], send_sem=l_ss.at[part, dst], recv_sem=l_rs.at[part, src_dev],
            device_id={'orb': dst}, device_id_type=MESH_ID)

    def if_last(dst, act):
        pl.when(dst <= n_tiles * extra)(act)

    def g_copy(dst, src_dev):
        return pltpu.make_async_remote_copy(
            src_ref=gsend, dst_ref=grecv.at[src_dev], send_sem=g_ss.at[dst], recv_sem=g_rs.at[src_dev],
            device_id={'orb': dst}, device_id_type=MESH_ID)

    def j_copy(dst, src_dev):
        return pltpu.make_async_remote_copy(
            src_ref=jsend.at[dst], dst_ref=jrecv.at[src_dev], send_sem=j_ss.at[dst], recv_sem=j_rs.at[src_dev],
            device_id={'aux': dst}, device_id_type=MESH_ID)

    def k_copy(orb, aux, src_dev):
        slot = aux * n_orb + orb
        return pltpu.make_async_remote_copy(
            src_ref=ksend.at[slot], dst_ref=krecv.at[src_dev], send_sem=k_ss.at[slot], recv_sem=k_rs.at[src_dev],
            device_id={'orb': orb, 'aux': aux}, device_id_type=MESH_ID)

    def ex_row(slot, m, tail):
        if slot == pairs:
            return last_row + m
        return (pairs * whole + slot * rest + m - whole) if tail else (slot * whole + m)

    last_row = rup(pairs * row_blk, SUBL)

    def t_part(count, m, at, mg, tail):

        def rows_of(m):
            return [bv[m, 0:q_main, :], bv[m, q_main:q_loc, :], jnp.zeros((left_pad - q_left, n_bf), jnp.float32)]

        def put(m, at_m, block, left):
            for d in range(n_orb):
                for t in range(n_tiles):
                    piece = block[d * SUBL:d * SUBL + occ_each, t * LANES:(t + 1) * LANES]
                    send[d, pl.ds(at_m + t * occ_each * mg, occ_each, stride=mg), :] = piece
                    if d // extra == t:
                        pick = d * SUBL + occ_each
                        ex_send[d, pl.ds(ex_row(pairs, m, tail), 1), :] = block[pick:pick + 1, t * LANES:(t + 1) * LANES]
            total = left[0:rows_l]
            for j in range(1, fold):
                total = total + pltpu.roll(left[j * rows_l:(j + 1) * rows_l], j * left_pad, 1)
            for d in range(n_orb):
                for u in range(pairs):
                    ex_send[d, pl.ds(ex_row(u, m, tail), 1), :] = total[d * pairs + u:d * pairs + u + 1]
            d = n_tiles * extra
            ex_send[d, pl.ds(ex_row(pairs, m, tail), 1), :] = total[n_orb * pairs:n_orb * pairs + 1]

        rows = jnp.concatenate(sum([rows_of(m + j) for j in range(count)], []), axis=0)
        block = mm(rows, ctn[...], 1, 0)
        for j in range(count):
            top = j * (q_main + left_pad)
            left = block[top + q_main:top + q_main + left_pad, LANES:]
            left = jnp.concatenate([left, jnp.zeros((LANES - left_pad, LANES), jnp.float32)], axis=0)
            put(m + j, at + j, block[top:top + q_main, 0:LANES].T, left.T)

    def t_send(is_small, k):
        for r in ORDER:
            t_copy(is_small, k, peer_orb(r), me).start()

    def t_small():
        small_load(0).wait()

        def step(j, carry):
            t_part(SMALL_STEP, whole + j * SMALL_STEP, j * SMALL_STEP, rest, True)
            return carry

        lax.fori_loop(0, rest // SMALL_STEP, step, 0)
        pl.semaphore_wait(barrier, n_orb - 1 + n_aux - 1)
        t_send(True, 0)

    def t_whole(k, carry):
        @pl.when(k < n_whole - 1)
        def _():
            whole_load(k).wait()

        def step(j, inner):
            t_part(WHOLE_STEP, k * SUBL + j * WHOLE_STEP, n_small * small_rows + k * whole_rows + j * WHOLE_STEP, SUBL, False)
            return inner

        lax.fori_loop(0, SUBL // WHOLE_STEP, step, 0)
        t_send(False, k)

        @pl.when(k == n_whole - 2)
        def _():
            gamma_part()
        return carry

    def gamma_part():
        whole_load(n_whole - 1).wait()
        pick = lax.broadcasted_iota(jnp.int32, (row_blk, n_bf), 0)
        pick_col = lax.broadcasted_iota(jnp.int32, (row_blk, n_bf), 1)
        own = mm((pick + me * row_blk == pick_col).astype(jnp.float32), occ_t, 1, 1)
        dens[...] = mm(own, occ_t, 1, 0)
        q_step = 5 * SUBL
        for q0 in range(0, q_loc, q_step):
            n_q = min(q_step, q_loc - q0)

            def body(m, acc):
                return acc + bv[m, q0:q0 + n_q, :] * dens[pl.ds(m, 1), :]

            srow[q0:q0 + n_q, :] = lax.fori_loop(0, row_blk, body, jnp.zeros((n_q, n_bf), jnp.float32), unroll=3)
        total = jnp.zeros(gsend.shape, jnp.float32)
        for k in range(srow.shape[0] // LANES):
            row_k = (lax.broadcasted_iota(jnp.int32, (gsend.shape[0], n_bf), 0) == k).astype(jnp.float32)
            total = total + mm(row_k, srow[k * LANES:(k + 1) * LANES, :], 1, 1)
        gsend[...] = total
        grecv[me] = total
        for r in ORDER:
            g_copy(peer_orb(r), me).start()

    def coulomb():
        for r in range(1, n_orb):
            g_copy(me, peer_orb(r)).wait_recv()
        gam = grecv[0]
        for src in range(1, n_orb):
            gam = gam + grecv[src]
        for k in range(srow.shape[0] // LANES):
            row_k = (lax.broadcasted_iota(jnp.int32, (gsend.shape[0], n_bf), 0) == k).astype(jnp.float32)
            gbc[k * LANES:(k + 1) * LANES, :] = mm(gam, row_k, 0, 0)

        def body(m, carry):
            jrows[pl.ds(m, 1), 0:n_bf] = jnp.sum(bv[m] * gbc[0:q_loc, :], axis=0, keepdims=True)
            return carry

        lax.fori_loop(0, row_blk, body, 0)
        jpad = jrows[...]
        for a in range(n_aux):
            piece = jpad if a == 0 else pltpu.roll(jpad, 2 * LANES - a * n_cols, 1)
            jsend[a] = piece[:, 0:LANES]
        jrecv[my] = jsend[my]
        for r in range(1, n_aux):
            j_copy(lax.rem(my + r, n_aux), my).start()

    def collect():
        recv[me] = send[me]
        for r in range(1, n_orb):
            t_copy(True, 0, me, peer_orb(r)).wait_recv()

        def last_rows(src, carry):
            for s in range(slots):
                xa[src, whole:row_blk, s * LANES:(s + 1) * LANES] = recv[src, s * rest:(s + 1) * rest, :]
            return carry

        lax.fori_loop(0, n_orb, last_rows, 0)

        def one_whole(k, carry):
            for r in range(1, n_orb):
                t_copy(False, k, me, peer_orb(r)).wait_recv()

            def tiles(src, inner):
                for s in range(slots):
                    at = pl.multiple_of(n_small * small_rows + k * whole_rows + s * SUBL, SUBL)
                    xa[src, pl.ds(pl.multiple_of(k * SUBL, SUBL), SUBL), s * LANES:(s + 1) * LANES] = recv[src, pl.ds(at, SUBL), :]
                return inner

            lax.fori_loop(0, n_orb, tiles, 0)
            return carry

        lax.fori_loop(0, n_whole, one_whole, 0)

    def collect_left(part):
        for r in range(1, n_orb):
            if part == 0:
                l_copy(0, me, peer_orb(r)).wait_recv()
            else:
                if_last(me, l_copy(1, me, peer_orb(r)).wait_recv)
        for src in range(n_orb):
            for s in range(pairs) if part == 0 else (pairs,):
                cols = slice((slots + s) * LANES, (slots + s + 1) * LANES)
                at = ex_row(s, 0, False)
                xa[src, 0:whole, cols] = ex_recv[src, at:at + whole, :]
                at = ex_row(s, whole, True)
                xa[src, whole:row_blk, cols] = ex_recv[src, at:at + rest, :]

    t_small()
    lax.fori_loop(0, n_whole, t_whole, 0)
    for r in ORDER:
        l_copy(0, peer_orb(r), me).start()
    for r in ORDER:
        if_last(peer_orb(r), l_copy(1, peer_orb(r), me).start)
    ex_recv[me] = ex_send[me]
    xa[...] = jnp.zeros(xa.shape, jnp.float32)
    coulomb()
    collect()
    kacc[...] = jnp.zeros(kacc.shape, jnp.float32)
    depth = 2 * LANES
    n_main = slots * LANES // depth

    def k_step(k, carry):
        @pl.when(k == n_main)
        def _():
            collect_left(0)

        @pl.when(k == n_main + 1)
        def _():
            collect_left(1)

        part = xa[:, :, pl.ds(pl.multiple_of(k * depth, depth), depth)].reshape(n_orb * row_pad, depth)
        kacc[...] += mm(part, part, 1, 1)
        return carry

    lax.fori_loop(0, n_main + 2, k_step, 0)

    half = row_pad // 2
    low_half = lax.broadcasted_iota(jnp.int32, (half, LANES), 1) < LANES // 2
    for orb in range(n_orb):
        for ctile in range(n_aux // 2):
            blk = kacc[orb * row_pad:(orb + 1) * row_pad, ctile * LANES:(ctile + 1) * LANES]
            top, bot = blk[0:half], blk[half:]
            ksend[2 * ctile * n_orb + orb] = jnp.where(low_half, top, pltpu.roll(bot, LANES // 2, 1))
            ksend[(2 * ctile + 1) * n_orb + orb] = jnp.where(low_half, pltpu.roll(top, LANES // 2, 1), bot)
    dev = my * n_orb + me
    krecv[dev] = ksend[dev]

    def hops(step, ring):
        return min(step, ring - step)

    steps = sorted(range(1, n_dev), key=lambda k: -(hops((k % n_orb + 1) // 2, n_orb // 2) + hops(k // n_orb, n_aux)))

    def k_out(step):
        return k_copy(peer_orb(step % n_orb), lax.rem(my + step // n_orb, n_aux), dev)

    for step in steps:
        k_out(step).start()
    for is_small, k in t_groups:
        for r in range(1, n_orb):
            t_copy(is_small, k, peer_orb(r), me).wait_send()
    for r in range(1, n_orb):
        l_copy(0, peer_orb(r), me).wait_send()
        if_last(peer_orb(r), l_copy(1, peer_orb(r), me).wait_send)
        g_copy(peer_orb(r), me).wait_send()
    for r in range(1, n_aux):
        j_copy(lax.rem(my + r, n_aux), my).wait_send()
    for r in range(1, n_aux):
        j_copy(my, lax.rem(my + r, n_aux)).wait_recv()
    jsum = jrecv[0]
    for src in range(1, n_aux):
        jsum = jsum + jrecv[src]

    for step in reversed(steps):
        k_copy(me, my, lax.rem(my + step // n_orb, n_aux) * n_orb + peer_orb(step % n_orb)).wait_recv()
    ksum = krecv[0]
    for src in range(1, n_dev):
        ksum = ksum + krecv[src]
    kblk = jnp.concatenate([ksum, pltpu.roll(ksum, LANES // 2, 1)], axis=0)
    pad_cols = row_pad - row_blk
    kcols = jnp.where(lax.broadcasted_iota(jnp.int32, (row_pad, LANES), 1) < row_blk, kblk, pltpu.roll(kblk, LANES - pad_cols, 1))
    out = 2.0 * jsum - kcols
    out_ref[...] = out[0:row_blk, 0:n_cols]

    for step in steps:
        k_out(step).wait_send()


def solution(mesh):
    n_orb = mesh.shape['orb']
    n_aux = mesh.shape['aux']

    def local_fock(fit_loc, orbitals):
        q_loc, row_blk, n_bf = fit_loc.shape
        n_occ = orbitals.shape[1]
        n_cols = n_bf // n_aux
        row_pad = rup(row_blk, SUBL)
        occ_each = n_occ // n_orb
        q_main = q_loc // LANES * LANES
        n_tiles = q_main // LANES
        slots = n_tiles * occ_each
        whole = row_blk // SUBL * SUBL
        left_pad = rup(q_loc - q_main, SUBL)
        fold = LANES // left_pad
        pairs = occ_each // fold
        extra = n_occ - n_orb * occ_each
        base = slots * row_blk
        rest = row_blk - whole
        assert n_orb == 2 * n_aux and n_cols == 2 * row_blk and occ_each % fold == 0 and occ_each < SUBL
        assert 0 < extra <= fold and (n_tiles + 1) * extra <= n_orb + 1 and row_pad * n_orb == 2 * LANES
        dims = (n_orb, n_aux, q_loc, row_blk, n_bf, n_occ, row_pad, occ_each, q_main, left_pad, fold, n_cols)
        n_dev = n_orb * n_aux
        n_groups = 1 + whole // SUBL
        assert rest % SMALL_STEP == 0 and slots * rest % SUBL == 0 and slots % 2 == 0 and pairs == 2
        ex_rows = rup(pairs * row_blk, SUBL) + rup(row_blk, SUBL)
        q_lanes = rup(q_loc, LANES)
        g_rows = rup(q_lanes // LANES, 4)
        f32 = jnp.float32
        dma = pltpu.SemaphoreType.DMA
        scratch = [
            pltpu.VMEM((row_blk, q_loc, n_bf), f32),
            pltpu.VMEM((n_occ, n_bf), f32),
            pltpu.VMEM((n_bf, 2 * LANES), f32),
            pltpu.VMEM((row_blk, n_bf), f32),
            pltpu.VMEM((n_orb, base, LANES), f32),
            pltpu.VMEM((n_orb, base, LANES), f32),
            pltpu.VMEM((n_orb, ex_rows, LANES), f32),
            pltpu.VMEM((n_orb, ex_rows, LANES), f32),
            pltpu.VMEM((n_orb, row_pad, (slots + pairs + 2) * LANES), f32),
            pltpu.VMEM((n_orb * row_pad, n_orb * row_pad), f32),
            pltpu.VMEM((q_lanes, n_bf), f32),
            pltpu.VMEM((g_rows, LANES), f32),
            pltpu.VMEM((n_orb, g_rows, LANES), f32),
            pltpu.VMEM((q_lanes, n_bf), f32),
            pltpu.VMEM((row_pad, 2 * LANES), f32),
            pltpu.VMEM((n_aux, row_pad, LANES), f32),
            pltpu.VMEM((n_aux, row_pad, LANES), f32),
            pltpu.VMEM((n_dev, row_pad // 2, LANES), f32),
            pltpu.VMEM((n_dev, row_pad // 2, LANES), f32),
            dma((n_groups + 1,)), dma((n_groups, n_orb)), dma((n_groups, n_orb)), dma((2, n_orb)), dma((2, n_orb)),
            dma((n_orb,)), dma((n_orb,)), dma((n_aux,)), dma((n_aux,)), dma((n_dev,)), dma((n_dev,)),
        ]
        return pl.pallas_call(
            functools.partial(fock_kernel, dims),
            out_shape=jax.ShapeDtypeStruct((row_blk, n_cols), f32),
            in_specs=[pl.BlockSpec(memory_space=pltpu.HBM)] * 2,
            out_specs=pl.BlockSpec(memory_space=pltpu.VMEM),
            scratch_shapes=scratch,
            compiler_params=pltpu.CompilerParams(collective_id=0, has_side_effects=True, vmem_limit_bytes=32 * 1024 * 1024),
            name='fock_build',
        )(pltpu.with_memory_space_constraint(jnp.transpose(fit_loc, (1, 0, 2)), pltpu.HBM), pltpu.with_memory_space_constraint(orbitals.T, pltpu.HBM))

    spec_fit = P(('sys', 'aux'), 'orb', None)
    spec_orbitals = P('sys', None)
    spec_out = P(('sys', 'orb'), 'aux')
    return jax.shard_map(local_fock, mesh=mesh, in_specs=(spec_fit, spec_orbitals), out_specs=spec_out, check_vma=False)
```

```python
import functools
import jax
import jax.numpy as jnp
from jax import lax
from jax.experimental import pallas as pl
from jax.experimental.pallas import tpu as pltpu
from jax.sharding import PartitionSpec as P

PREC_MODE = lax.Precision.HIGHEST
MESH_ID = pl.DeviceIdType.MESH
LANES = 128
SUBL = 8


ORDER = ((2, 0), (2, 1), (1, 0), (3, 0), (1, 1), (3, 1), (0, 1))
SMALL_STEP = 6
WHOLE_STEP = 8


def mm(lhs, rhs, lhs_dim, rhs_dim):
    return lax.dot_general(lhs, rhs, (((lhs_dim,), (rhs_dim,)), ((), ())), precision=PREC_MODE, preferred_element_type=jnp.float32)


def rup(value, unit):
    return -(-value // unit) * unit


def fock_kernel(dims, fit_ref, occ_ref, out_ref, bv, ct, ctn, dens, recv, send, ex_recv, ex_send, xa, kacc,
                srow, gsend, grecv, gbc, jrows, jsend, jrecv, ksend, krecv,
                load_sem, t_ss, t_rs, l_ss, l_rs, g_ss, g_rs, j_ss, j_rs, k_ss, k_rs):
    (n_orb, n_aux, q_loc, row_blk, n_bf, n_occ, row_pad, occ_each, q_main, left_pad, fold, n_cols) = dims
    me = lax.axis_index('orb')
    my = lax.axis_index('aux')
    n_dev = n_orb * n_aux
    n_tiles = q_main // LANES
    slots = n_tiles * occ_each
    q_left = q_loc - q_main
    whole = row_blk // SUBL * SUBL
    rest = row_blk - whole
    pairs = occ_each // fold
    extra = n_occ - n_orb * occ_each

    def peer_orb(step):
        return lax.rem(me + step, n_orb)

    chip, core = me // 2, lax.rem(me, 2)
    n_chips = n_orb // 2

    def peer_at(place):
        ahead, flip = place
        return lax.rem(chip + ahead, n_chips) * 2 + (1 - core if flip else core)

    n_small = 1
    n_whole = whole // SUBL
    n_groups = n_small + n_whole
    small_rows, whole_rows = slots * rest, slots * SUBL

    def load(first, count, sem):
        return pltpu.make_async_copy(fit_ref.at[pl.ds(first, count)], bv.at[pl.ds(first, count)], load_sem.at[sem])

    def small_load(k):
        return load(whole, rest, k)

    def whole_load(k):
        return load(k * SUBL, SUBL, n_small + k)

    occ_load = pltpu.make_async_copy(occ_ref, ct, load_sem.at[n_groups])
    occ_load.start()
    for k in range(n_small):
        small_load(k).start()

    barrier = pltpu.get_barrier_semaphore()

    for r in range(1, n_orb):
        pl.semaphore_signal(barrier, inc=1, device_id={'orb': peer_orb(r)}, device_id_type=MESH_ID)
    for r in range(1, n_aux):
        pl.semaphore_signal(barrier, inc=1, device_id={'aux': lax.rem(my + r, n_aux)}, device_id_type=MESH_ID)
    ex_send[...] = jnp.zeros(ex_send.shape, jnp.float32)

    occ_load.wait()
    occ_t = ct[...]
    rows_l = rup(pairs * n_orb + 1, SUBL)
    row = lax.broadcasted_iota(jnp.int32, (n_occ, LANES), 0)
    col = lax.broadcasted_iota(jnp.int32, (n_occ, LANES), 1)
    in_blk = col % SUBL
    which = (((in_blk < occ_each) & (row == col // SUBL * occ_each + in_blk))
             | ((in_blk == occ_each) & (row == n_orb * occ_each + col // SUBL % extra))) & (col < n_orb * SUBL)
    ctn[:, 0:LANES] = mm(occ_t, which.astype(jnp.float32), 0, 0)
    in_blk = col % rows_l
    which = (in_blk <= pairs * n_orb) & (row == in_blk * fold + col // rows_l) & (col < fold * rows_l)
    ctn[:, LANES:] = mm(occ_t, which.astype(jnp.float32), 0, 0)
    def t_copy(is_small, k, dst, src_dev):
        rows = pl.ds(pl.multiple_of(k * small_rows, SUBL), small_rows) if is_small else pl.ds(pl.multiple_of(n_small * small_rows + k * whole_rows, SUBL), whole_rows)
        g = k if is_small else n_small + k
        return pltpu.make_async_remote_copy(
            src_ref=send.at[dst, rows], dst_ref=recv.at[src_dev, rows],
            send_sem=t_ss.at[g, dst], recv_sem=t_rs.at[g, src_dev], device_id={'orb': dst}, device_id_type=MESH_ID)

    t_groups = [(True, k) for k in range(n_small)] + [(False, k) for k in range(n_whole)]

    def l_copy(part, dst, src_dev):
        rows = pl.ds(0, last_row) if part == 0 else pl.ds(last_row, ex_send.shape[1] - last_row)
        return pltpu.make_async_remote_copy(
            src_ref=ex_send.at[dst, rows], dst_ref=ex_recv.at[src_dev, rows], send_sem=l_ss.at[part, dst], recv_sem=l_rs.at[part, src_dev],
            device_id={'orb': dst}, device_id_type=MESH_ID)

    def if_last(dst, act):
        pl.when(dst <= n_tiles * extra)(act)

    def g_copy(dst, src_dev):
        return pltpu.make_async_remote_copy(
            src_ref=gsend, dst_ref=grecv.at[src_dev], send_sem=g_ss.at[dst], recv_sem=g_rs.at[src_dev],
            device_id={'orb': dst}, device_id_type=MESH_ID)

    def j_copy(dst, src_dev):
        return pltpu.make_async_remote_copy(
            src_ref=jsend.at[dst], dst_ref=jrecv.at[src_dev], send_sem=j_ss.at[dst], recv_sem=j_rs.at[src_dev],
            device_id={'aux': dst}, device_id_type=MESH_ID)

    def k_copy(orb, aux, src_dev):
        slot = aux * n_orb + orb
        return pltpu.make_async_remote_copy(
            src_ref=ksend.at[slot], dst_ref=krecv.at[src_dev], send_sem=k_ss.at[slot], recv_sem=k_rs.at[src_dev],
            device_id={'orb': orb, 'aux': aux}, device_id_type=MESH_ID)

    def ex_row(slot, m, tail):
        if slot == pairs:
            return last_row + m
        return (pairs * whole + slot * rest + m - whole) if tail else (slot * whole + m)

    last_row = rup(pairs * row_blk, SUBL)

    def t_part(count, m, at, mg, tail):

        def rows_of(m):
            return [bv[m, 0:q_main, :], bv[m, q_main:q_loc, :], jnp.zeros((left_pad - q_left, n_bf), jnp.float32)]

        def put(m, at_m, block, left):
            for d in range(n_orb):
                for t in range(n_tiles):
                    piece = block[d * SUBL:d * SUBL + occ_each, t * LANES:(t + 1) * LANES]
                    send[d, pl.ds(at_m + t * occ_each * mg, occ_each, stride=mg), :] = piece
                    if d // extra == t:
                        pick = d * SUBL + occ_each
                        ex_send[d, pl.ds(ex_row(pairs, m, tail), 1), :] = block[pick:pick + 1, t * LANES:(t + 1) * LANES]
            total = left[0:rows_l]
            for j in range(1, fold):
                total = total + pltpu.roll(left[j * rows_l:(j + 1) * rows_l], j * left_pad, 1)
            for d in range(n_orb):
                for u in range(pairs):
                    ex_send[d, pl.ds(ex_row(u, m, tail), 1), :] = total[d * pairs + u:d * pairs + u + 1]
            d = n_tiles * extra
            ex_send[d, pl.ds(ex_row(pairs, m, tail), 1), :] = total[n_orb * pairs:n_orb * pairs + 1]

        rows = jnp.concatenate(sum([rows_of(m + j) for j in range(count)], []), axis=0)
        block = mm(rows, ctn[...], 1, 0)
        for j in range(count):
            top = j * (q_main + left_pad)
            left = block[top + q_main:top + q_main + left_pad, LANES:]
            left = jnp.concatenate([left, jnp.zeros((LANES - left_pad, LANES), jnp.float32)], axis=0)
            put(m + j, at + j, block[top:top + q_main, 0:LANES].T, left.T)

    def t_send(is_small, k):
        for r in ORDER:
            t_copy(is_small, k, peer_at(r), me).start()

    def t_small():
        small_load(0).wait()
        for k in range(n_whole):
            whole_load(k).start()

        def step(j, carry):
            t_part(SMALL_STEP, whole + j * SMALL_STEP, j * SMALL_STEP, rest, True)
            return carry

        lax.fori_loop(0, rest // SMALL_STEP, step, 0)
        pl.semaphore_wait(barrier, n_orb - 1 + n_aux - 1)
        t_send(True, 0)

    def t_whole(k, carry):
        @pl.when(k < n_whole - 1)
        def _():
            whole_load(k).wait()

        def step(j, inner):
            t_part(WHOLE_STEP, k * SUBL + j * WHOLE_STEP, n_small * small_rows + k * whole_rows + j * WHOLE_STEP, SUBL, False)
            return inner

        lax.fori_loop(0, SUBL // WHOLE_STEP, step, 0)
        t_send(False, k)

        @pl.when(k == n_whole - 2)
        def _():
            gamma_part()
        return carry

    def gamma_part():
        whole_load(n_whole - 1).wait()
        pick = lax.broadcasted_iota(jnp.int32, (row_blk, n_bf), 0)
        pick_col = lax.broadcasted_iota(jnp.int32, (row_blk, n_bf), 1)
        own = mm((pick + me * row_blk == pick_col).astype(jnp.float32), occ_t, 1, 1)
        dens[...] = mm(own, occ_t, 1, 0)
        q_step = 5 * SUBL
        for q0 in range(0, q_loc, q_step):
            n_q = min(q_step, q_loc - q0)

            def body(m, acc):
                return acc + bv[m, q0:q0 + n_q, :] * dens[pl.ds(m, 1), :]

            srow[q0:q0 + n_q, :] = lax.fori_loop(0, row_blk, body, jnp.zeros((n_q, n_bf), jnp.float32), unroll=3)
        total = jnp.zeros(gsend.shape, jnp.float32)
        for k in range(srow.shape[0] // LANES):
            row_k = (lax.broadcasted_iota(jnp.int32, (gsend.shape[0], n_bf), 0) == k).astype(jnp.float32)
            total = total + mm(row_k, srow[k * LANES:(k + 1) * LANES, :], 1, 1)
        gsend[...] = total
        grecv[me] = total
        for r in ORDER:
            g_copy(peer_at(r), me).start()

    def coulomb():
        for r in range(1, n_orb):
            g_copy(me, peer_orb(r)).wait_recv()
        gam = grecv[0]
        for src in range(1, n_orb):
            gam = gam + grecv[src]
        for k in range(srow.shape[0] // LANES):
            row_k = (lax.broadcasted_iota(jnp.int32, (gsend.shape[0], n_bf), 0) == k).astype(jnp.float32)
            gbc[k * LANES:(k + 1) * LANES, :] = mm(gam, row_k, 0, 0)

        def body(m, carry):
            jrows[pl.ds(m, 1), 0:n_bf] = jnp.sum(bv[m] * gbc[0:q_loc, :], axis=0, keepdims=True)
            return carry

        lax.fori_loop(0, row_blk, body, 0)
        jpad = jrows[...]
        for a in range(n_aux):
            piece = jpad if a == 0 else pltpu.roll(jpad, 2 * LANES - a * n_cols, 1)
            jsend[a] = piece[:, 0:LANES]
        jrecv[my] = jsend[my]
        for r in range(1, n_aux):
            j_copy(lax.rem(my + r, n_aux), my).start()

    def collect():
        recv[me] = send[me]
        for r in range(1, n_orb):
            t_copy(True, 0, me, peer_orb(r)).wait_recv()

        def last_rows(src, carry):
            for s in range(slots):
                xa[src, whole:row_blk, s * LANES:(s + 1) * LANES] = recv[src, s * rest:(s + 1) * rest, :]
            return carry

        lax.fori_loop(0, n_orb, last_rows, 0)

        def one_whole(k, carry):
            for r in range(1, n_orb):
                t_copy(False, k, me, peer_orb(r)).wait_recv()

            def tiles(src, inner):
                for s in range(slots):
                    at = pl.multiple_of(n_small * small_rows + k * whole_rows + s * SUBL, SUBL)
                    xa[src, pl.ds(pl.multiple_of(k * SUBL, SUBL), SUBL), s * LANES:(s + 1) * LANES] = recv[src, pl.ds(at, SUBL), :]
                return inner

            lax.fori_loop(0, n_orb, tiles, 0)
            return carry

        lax.fori_loop(0, n_whole, one_whole, 0)

    def collect_left(part):
        for r in range(1, n_orb):
            if part == 0:
                l_copy(0, me, peer_orb(r)).wait_recv()
            else:
                if_last(me, l_copy(1, me, peer_orb(r)).wait_recv)
        for src in range(n_orb):
            for s in range(pairs) if part == 0 else (pairs,):
                cols = slice((slots + s) * LANES, (slots + s + 1) * LANES)
                at = ex_row(s, 0, False)
                xa[src, 0:whole, cols] = ex_recv[src, at:at + whole, :]
                at = ex_row(s, whole, True)
                xa[src, whole:row_blk, cols] = ex_recv[src, at:at + rest, :]

    t_small()
    lax.fori_loop(0, n_whole, t_whole, 0)
    for r in ORDER:
        l_copy(0, peer_at(r), me).start()
    for r in ORDER:
        if_last(peer_at(r), l_copy(1, peer_at(r), me).start)
    ex_recv[me] = ex_send[me]
    xa[...] = jnp.zeros(xa.shape, jnp.float32)
    coulomb()
    collect()
    kacc[...] = jnp.zeros(kacc.shape, jnp.float32)
    depth = 2 * LANES
    n_main = slots * LANES // depth

    def k_step(k, carry):
        @pl.when(k == n_main)
        def _():
            collect_left(0)

        @pl.when(k == n_main + 1)
        def _():
            collect_left(1)

        part = xa[:, :, pl.ds(pl.multiple_of(k * depth, depth), depth)].reshape(n_orb * row_pad, depth)
        kacc[...] += mm(part, part, 1, 1)
        return carry

    lax.fori_loop(0, n_main + 2, k_step, 0)

    half = row_pad // 2
    low_half = lax.broadcasted_iota(jnp.int32, (half, LANES), 1) < LANES // 2
    for orb in range(n_orb):
        for ctile in range(n_aux // 2):
            blk = kacc[orb * row_pad:(orb + 1) * row_pad, ctile * LANES:(ctile + 1) * LANES]
            top, bot = blk[0:half], blk[half:]
            ksend[2 * ctile * n_orb + orb] = jnp.where(low_half, top, pltpu.roll(bot, LANES // 2, 1))
            ksend[(2 * ctile + 1) * n_orb + orb] = jnp.where(low_half, pltpu.roll(top, LANES // 2, 1), bot)
    dev = my * n_orb + me
    krecv[dev] = ksend[dev]

    def hops(step, ring):
        return min(step, ring - step)

    steps = [(ahead, flip, up) for ahead in range(n_chips) for flip in range(2) for up in range(n_aux)][1:]
    steps = sorted(steps, key=lambda p: -(hops(p[0], n_chips) + hops(p[2], n_aux)))

    def k_out(step):
        return k_copy(peer_at(step[:2]), lax.rem(my + step[2], n_aux), dev)

    for step in steps:
        k_out(step).start()
    for is_small, k in t_groups:
        for r in range(1, n_orb):
            t_copy(is_small, k, peer_orb(r), me).wait_send()
    for r in range(1, n_orb):
        l_copy(0, peer_orb(r), me).wait_send()
        if_last(peer_orb(r), l_copy(1, peer_orb(r), me).wait_send)
        g_copy(peer_orb(r), me).wait_send()
    for r in range(1, n_aux):
        j_copy(lax.rem(my + r, n_aux), my).wait_send()
    for r in range(1, n_aux):
        j_copy(my, lax.rem(my + r, n_aux)).wait_recv()
    jsum = jrecv[0]
    for src in range(1, n_aux):
        jsum = jsum + jrecv[src]

    for step in reversed(steps):
        k_copy(me, my, lax.rem(my + step[2], n_aux) * n_orb + peer_at(step[:2])).wait_recv()
    ksum = krecv[0]
    for src in range(1, n_dev):
        ksum = ksum + krecv[src]
    kblk = jnp.concatenate([ksum, pltpu.roll(ksum, LANES // 2, 1)], axis=0)
    pad_cols = row_pad - row_blk
    kcols = jnp.where(lax.broadcasted_iota(jnp.int32, (row_pad, LANES), 1) < row_blk, kblk, pltpu.roll(kblk, LANES - pad_cols, 1))
    out = 2.0 * jsum - kcols
    out_ref[...] = out[0:row_blk, 0:n_cols]

    for step in steps:
        k_out(step).wait_send()


def solution(mesh):
    n_orb = mesh.shape['orb']
    n_aux = mesh.shape['aux']

    def local_fock(fit_loc, orbitals):
        q_loc, row_blk, n_bf = fit_loc.shape
        n_occ = orbitals.shape[1]
        n_cols = n_bf // n_aux
        row_pad = rup(row_blk, SUBL)
        occ_each = n_occ // n_orb
        q_main = q_loc // LANES * LANES
        n_tiles = q_main // LANES
        slots = n_tiles * occ_each
        whole = row_blk // SUBL * SUBL
        left_pad = rup(q_loc - q_main, SUBL)
        fold = LANES // left_pad
        pairs = occ_each // fold
        extra = n_occ - n_orb * occ_each
        base = slots * row_blk
        rest = row_blk - whole
        assert n_orb == 2 * n_aux and n_cols == 2 * row_blk and occ_each % fold == 0 and occ_each < SUBL
        assert 0 < extra <= fold and (n_tiles + 1) * extra <= n_orb + 1 and row_pad * n_orb == 2 * LANES
        dims = (n_orb, n_aux, q_loc, row_blk, n_bf, n_occ, row_pad, occ_each, q_main, left_pad, fold, n_cols)
        n_dev = n_orb * n_aux
        n_groups = 1 + whole // SUBL
        assert len(ORDER) == n_orb - 1 and rest % SMALL_STEP == 0 and slots * rest % SUBL == 0 and slots % 2 == 0 and pairs == 2
        ex_rows = rup(pairs * row_blk, SUBL) + rup(row_blk, SUBL)
        q_lanes = rup(q_loc, LANES)
        g_rows = rup(q_lanes // LANES, 4)
        f32 = jnp.float32
        dma = pltpu.SemaphoreType.DMA
        scratch = [
            pltpu.VMEM((row_blk, q_loc, n_bf), f32),
            pltpu.VMEM((n_occ, n_bf), f32),
            pltpu.VMEM((n_bf, 2 * LANES), f32),
            pltpu.VMEM((row_blk, n_bf), f32),
            pltpu.VMEM((n_orb, base, LANES), f32),
            pltpu.VMEM((n_orb, base, LANES), f32),
            pltpu.VMEM((n_orb, ex_rows, LANES), f32),
            pltpu.VMEM((n_orb, ex_rows, LANES), f32),
            pltpu.VMEM((n_orb, row_pad, (slots + pairs + 2) * LANES), f32),
            pltpu.VMEM((n_orb * row_pad, n_orb * row_pad), f32),
            pltpu.VMEM((q_lanes, n_bf), f32),
            pltpu.VMEM((g_rows, LANES), f32),
            pltpu.VMEM((n_orb, g_rows, LANES), f32),
            pltpu.VMEM((q_lanes, n_bf), f32),
            pltpu.VMEM((row_pad, 2 * LANES), f32),
            pltpu.VMEM((n_aux, row_pad, LANES), f32),
            pltpu.VMEM((n_aux, row_pad, LANES), f32),
            pltpu.VMEM((n_dev, row_pad // 2, LANES), f32),
            pltpu.VMEM((n_dev, row_pad // 2, LANES), f32),
            dma((n_groups + 1,)), dma((n_groups, n_orb)), dma((n_groups, n_orb)), dma((2, n_orb)), dma((2, n_orb)),
            dma((n_orb,)), dma((n_orb,)), dma((n_aux,)), dma((n_aux,)), dma((n_dev,)), dma((n_dev,)),
        ]
        return pl.pallas_call(
            functools.partial(fock_kernel, dims),
            out_shape=jax.ShapeDtypeStruct((row_blk, n_cols), f32),
            in_specs=[pl.BlockSpec(memory_space=pltpu.HBM)] * 2,
            out_specs=pl.BlockSpec(memory_space=pltpu.VMEM),
            scratch_shapes=scratch,
            compiler_params=pltpu.CompilerParams(collective_id=0, has_side_effects=True, vmem_limit_bytes=32 * 1024 * 1024),
            name='fock_build',
        )(pltpu.with_memory_space_constraint(jnp.transpose(fit_loc, (1, 0, 2)), pltpu.HBM), pltpu.with_memory_space_constraint(orbitals.T, pltpu.HBM))

    spec_fit = P(('sys', 'aux'), 'orb', None)
    spec_orbitals = P('sys', None)
    spec_out = P(('sys', 'orb'), 'aux')
    return jax.shard_map(local_fock, mesh=mesh, in_specs=(spec_fit, spec_orbitals), out_specs=spec_out, check_vma=False)
```

```python
import functools
import jax
import jax.numpy as jnp
from jax import lax
from jax.experimental import pallas as pl
from jax.experimental.pallas import tpu as pltpu
from jax.sharding import PartitionSpec as P

PREC_MODE = lax.Precision.HIGHEST
MESH_ID = pl.DeviceIdType.MESH
LANES = 128
SUBL = 8


ORDER = ((2, 0), (2, 1), (1, 0), (3, 0), (1, 1), (3, 1), (0, 1))
SMALL_STEP = 6
WHOLE_STEP = 8


def mm(lhs, rhs, lhs_dim, rhs_dim):
    return lax.dot_general(lhs, rhs, (((lhs_dim,), (rhs_dim,)), ((), ())), precision=PREC_MODE, preferred_element_type=jnp.float32)


def rup(value, unit):
    return -(-value // unit) * unit


def fock_kernel(dims, fit_ref, occ_ref, out_ref, bv, ct, ctn, dens, recv, send, ex_recv, ex_send, xa, kacc,
                srow, gsend, grecv, gbc, jrows, jsend, jrecv, ksend, krecv,
                load_sem, t_ss, t_rs, l_ss, l_rs, g_ss, g_rs, j_ss, j_rs, k_ss, k_rs):
    (n_orb, n_aux, q_loc, row_blk, n_bf, n_occ, row_pad, occ_each, q_main, left_pad, fold, n_cols) = dims
    me = lax.axis_index('orb')
    my = lax.axis_index('aux')
    n_dev = n_orb * n_aux
    n_tiles = q_main // LANES
    slots = n_tiles * occ_each
    q_left = q_loc - q_main
    whole = row_blk // SUBL * SUBL
    rest = row_blk - whole
    pairs = occ_each // fold
    extra = n_occ - n_orb * occ_each

    def peer_orb(step):
        return lax.rem(me + step, n_orb)

    chip, core = me // 2, lax.rem(me, 2)
    n_chips = n_orb // 2

    def peer_at(place):
        ahead, flip = place
        return lax.rem(chip + ahead, n_chips) * 2 + (1 - core if flip else core)

    n_small = 1
    n_whole = whole // SUBL
    n_groups = n_small + n_whole
    small_rows, whole_rows = slots * rest, slots * SUBL

    def load(first, count, sem):
        return pltpu.make_async_copy(fit_ref.at[pl.ds(first, count)], bv.at[pl.ds(first, count)], load_sem.at[sem])

    def small_load(k):
        return load(whole, rest, k)

    def whole_load(k):
        return load(k * SUBL, SUBL, n_small + k)

    barrier = pltpu.get_barrier_semaphore()

    for r in ORDER:
        pl.semaphore_signal(barrier, inc=1, device_id={'orb': peer_at(r)}, device_id_type=MESH_ID)
    for r in range(1, n_aux):
        pl.semaphore_signal(barrier, inc=1, device_id={'aux': lax.rem(my + r, n_aux)}, device_id_type=MESH_ID)
    occ_load = pltpu.make_async_copy(occ_ref, ct, load_sem.at[n_groups])
    occ_load.start()
    for k in range(n_small):
        small_load(k).start()

    ex_send[...] = jnp.zeros(ex_send.shape, jnp.float32)

    occ_load.wait()
    occ_t = ct[...]
    rows_l = rup(pairs * n_orb + 1, SUBL)
    row = lax.broadcasted_iota(jnp.int32, (n_occ, LANES), 0)
    col = lax.broadcasted_iota(jnp.int32, (n_occ, LANES), 1)
    in_blk = col % SUBL
    which = (((in_blk < occ_each) & (row == col // SUBL * occ_each + in_blk))
             | ((in_blk == occ_each) & (row == n_orb * occ_each + col // SUBL % extra))) & (col < n_orb * SUBL)
    ctn[:, 0:LANES] = mm(occ_t, which.astype(jnp.float32), 0, 0)
    in_blk = col % rows_l
    which = (in_blk <= pairs * n_orb) & (row == in_blk * fold + col // rows_l) & (col < fold * rows_l)
    ctn[:, LANES:] = mm(occ_t, which.astype(jnp.float32), 0, 0)
    def t_copy(is_small, k, dst, src_dev):
        rows = pl.ds(pl.multiple_of(k * small_rows, SUBL), small_rows) if is_small else pl.ds(pl.multiple_of(n_small * small_rows + k * whole_rows, SUBL), whole_rows)
        g = k if is_small else n_small + k
        return pltpu.make_async_remote_copy(
            src_ref=send.at[dst, rows], dst_ref=recv.at[src_dev, rows],
            send_sem=t_ss.at[g, dst], recv_sem=t_rs.at[g, src_dev], device_id={'orb': dst}, device_id_type=MESH_ID)

    t_groups = [(True, k) for k in range(n_small)] + [(False, k) for k in range(n_whole)]

    def l_copy(part, dst, src_dev):
        rows = pl.ds(0, last_row) if part == 0 else pl.ds(last_row, ex_send.shape[1] - last_row)
        return pltpu.make_async_remote_copy(
            src_ref=ex_send.at[dst, rows], dst_ref=ex_recv.at[src_dev, rows], send_sem=l_ss.at[part, dst], recv_sem=l_rs.at[part, src_dev],
            device_id={'orb': dst}, device_id_type=MESH_ID)

    def if_last(dst, act):
        pl.when(dst <= n_tiles * extra)(act)

    def g_copy(dst, src_dev):
        return pltpu.make_async_remote_copy(
            src_ref=gsend, dst_ref=grecv.at[src_dev], send_sem=g_ss.at[dst], recv_sem=g_rs.at[src_dev],
            device_id={'orb': dst}, device_id_type=MESH_ID)

    def j_copy(dst, src_dev):
        return pltpu.make_async_remote_copy(
            src_ref=jsend.at[dst], dst_ref=jrecv.at[src_dev], send_sem=j_ss.at[dst], recv_sem=j_rs.at[src_dev],
            device_id={'aux': dst}, device_id_type=MESH_ID)

    def k_copy(orb, aux, src_dev):
        slot = aux * n_orb + orb
        return pltpu.make_async_remote_copy(
            src_ref=ksend.at[slot], dst_ref=krecv.at[src_dev], send_sem=k_ss.at[slot], recv_sem=k_rs.at[src_dev],
            device_id={'orb': orb, 'aux': aux}, device_id_type=MESH_ID)

    def ex_row(slot, m, tail):
        if slot == pairs:
            return last_row + m
        return (pairs * whole + slot * rest + m - whole) if tail else (slot * whole + m)

    last_row = rup(pairs * row_blk, SUBL)

    def t_part(count, m, at, mg, tail):

        def rows_of(m):
            return [bv[m, 0:q_main, :], bv[m, q_main:q_loc, :], jnp.zeros((left_pad - q_left, n_bf), jnp.float32)]

        def put(m, at_m, block, left):
            for d in range(n_orb):
                for t in range(n_tiles):
                    piece = block[d * SUBL:d * SUBL + occ_each, t * LANES:(t + 1) * LANES]
                    send[d, pl.ds(at_m + t * occ_each * mg, occ_each, stride=mg), :] = piece
                    if d // extra == t:
                        pick = d * SUBL + occ_each
                        ex_send[d, pl.ds(ex_row(pairs, m, tail), 1), :] = block[pick:pick + 1, t * LANES:(t + 1) * LANES]
            total = left[0:rows_l]
            for j in range(1, fold):
                total = total + pltpu.roll(left[j * rows_l:(j + 1) * rows_l], j * left_pad, 1)
            for d in range(n_orb):
                for u in range(pairs):
                    ex_send[d, pl.ds(ex_row(u, m, tail), 1), :] = total[d * pairs + u:d * pairs + u + 1]
            d = n_tiles * extra
            ex_send[d, pl.ds(ex_row(pairs, m, tail), 1), :] = total[n_orb * pairs:n_orb * pairs + 1]

        rows = jnp.concatenate(sum([rows_of(m + j) for j in range(count)], []), axis=0)
        block = mm(rows, ctn[...], 1, 0)
        for j in range(count):
            top = j * (q_main + left_pad)
            left = block[top + q_main:top + q_main + left_pad, LANES:]
            left = jnp.concatenate([left, jnp.zeros((LANES - left_pad, LANES), jnp.float32)], axis=0)
            put(m + j, at + j, block[top:top + q_main, 0:LANES].T, left.T)

    def t_send(is_small, k):
        for r in ORDER:
            t_copy(is_small, k, peer_at(r), me).start()

    def t_small():
        small_load(0).wait()
        for k in range(n_whole):
            whole_load(k).start()

        def step(j, carry):
            t_part(SMALL_STEP, whole + j * SMALL_STEP, j * SMALL_STEP, rest, True)
            return carry

        lax.fori_loop(0, rest // SMALL_STEP, step, 0)
        pl.semaphore_wait(barrier, n_orb - 1 + n_aux - 1)
        t_send(True, 0)

    def t_whole(k, carry):
        @pl.when(k < n_whole - 1)
        def _():
            whole_load(k).wait()

        def step(j, inner):
            t_part(WHOLE_STEP, k * SUBL + j * WHOLE_STEP, n_small * small_rows + k * whole_rows + j * WHOLE_STEP, SUBL, False)
            return inner

        lax.fori_loop(0, SUBL // WHOLE_STEP, step, 0)
        t_send(False, k)

        @pl.when(k == n_whole - 2)
        def _():
            gamma_part()
        return carry

    def gamma_part():
        whole_load(n_whole - 1).wait()
        pick = lax.broadcasted_iota(jnp.int32, (row_blk, n_bf), 0)
        pick_col = lax.broadcasted_iota(jnp.int32, (row_blk, n_bf), 1)
        own = mm((pick + me * row_blk == pick_col).astype(jnp.float32), occ_t, 1, 1)
        dens[...] = mm(own, occ_t, 1, 0)
        q_step = 5 * SUBL
        for q0 in range(0, q_loc, q_step):
            n_q = min(q_step, q_loc - q0)

            def body(m, acc):
                return acc + bv[m, q0:q0 + n_q, :] * dens[pl.ds(m, 1), :]

            srow[q0:q0 + n_q, :] = lax.fori_loop(0, row_blk, body, jnp.zeros((n_q, n_bf), jnp.float32), unroll=3)
        total = jnp.zeros(gsend.shape, jnp.float32)
        for k in range(srow.shape[0] // LANES):
            row_k = (lax.broadcasted_iota(jnp.int32, (gsend.shape[0], n_bf), 0) == k).astype(jnp.float32)
            total = total + mm(row_k, srow[k * LANES:(k + 1) * LANES, :], 1, 1)
        gsend[...] = total
        grecv[me] = total
        for r in ORDER:
            g_copy(peer_at(r), me).start()

    def coulomb():
        for r in range(1, n_orb):
            g_copy(me, peer_orb(r)).wait_recv()
        gam = grecv[0]
        for src in range(1, n_orb):
            gam = gam + grecv[src]
        for k in range(srow.shape[0] // LANES):
            row_k = (lax.broadcasted_iota(jnp.int32, (gsend.shape[0], n_bf), 0) == k).astype(jnp.float32)
            gbc[k * LANES:(k + 1) * LANES, :] = mm(gam, row_k, 0, 0)

        def body(m, carry):
            jrows[pl.ds(m, 1), 0:n_bf] = jnp.sum(bv[m] * gbc[0:q_loc, :], axis=0, keepdims=True)
            return carry

        lax.fori_loop(0, row_blk, body, 0)
        jpad = jrows[...]
        for a in range(n_aux):
            piece = jpad if a == 0 else pltpu.roll(jpad, 2 * LANES - a * n_cols, 1)
            jsend[a] = piece[:, 0:LANES]
        jrecv[my] = jsend[my]
        for r in range(1, n_aux):
            j_copy(lax.rem(my + r, n_aux), my).start()

    def collect():
        recv[me] = send[me]
        for r in range(1, n_orb):
            t_copy(True, 0, me, peer_orb(r)).wait_recv()

        def last_rows(src, carry):
            for s in range(slots):
                xa[src, whole:row_blk, s * LANES:(s + 1) * LANES] = recv[src, s * rest:(s + 1) * rest, :]
            return carry

        lax.fori_loop(0, n_orb, last_rows, 0)

        def one_whole(k, carry):
            for r in range(1, n_orb):
                t_copy(False, k, me, peer_orb(r)).wait_recv()

            def tiles(src, inner):
                for s in range(slots):
                    at = pl.multiple_of(n_small * small_rows + k * whole_rows + s * SUBL, SUBL)
                    xa[src, pl.ds(pl.multiple_of(k * SUBL, SUBL), SUBL), s * LANES:(s + 1) * LANES] = recv[src, pl.ds(at, SUBL), :]
                return inner

            lax.fori_loop(0, n_orb, tiles, 0)
            return carry

        lax.fori_loop(0, n_whole, one_whole, 0)

    def collect_left(part):
        for r in range(1, n_orb):
            if part == 0:
                l_copy(0, me, peer_orb(r)).wait_recv()
            else:
                if_last(me, l_copy(1, me, peer_orb(r)).wait_recv)
        for src in range(n_orb):
            for s in range(pairs) if part == 0 else (pairs,):
                cols = slice((slots + s) * LANES, (slots + s + 1) * LANES)
                at = ex_row(s, 0, False)
                xa[src, 0:whole, cols] = ex_recv[src, at:at + whole, :]
                at = ex_row(s, whole, True)
                xa[src, whole:row_blk, cols] = ex_recv[src, at:at + rest, :]

    t_small()
    lax.fori_loop(0, n_whole, t_whole, 0)
    for r in ORDER:
        l_copy(0, peer_at(r), me).start()
    for r in ORDER:
        if_last(peer_at(r), l_copy(1, peer_at(r), me).start)
    ex_recv[me] = ex_send[me]
    xa[...] = jnp.zeros(xa.shape, jnp.float32)
    coulomb()
    collect()
    kacc[...] = jnp.zeros(kacc.shape, jnp.float32)
    depth = 2 * LANES
    n_main = slots * LANES // depth

    def k_step(k, carry):
        @pl.when(k == n_main)
        def _():
            collect_left(0)

        @pl.when(k == n_main + 1)
        def _():
            collect_left(1)

        part = xa[:, :, pl.ds(pl.multiple_of(k * depth, depth), depth)].reshape(n_orb * row_pad, depth)
        kacc[...] += mm(part, part, 1, 1)
        return carry

    lax.fori_loop(0, n_main + 2, k_step, 0)

    half = row_pad // 2
    low_half = lax.broadcasted_iota(jnp.int32, (half, LANES), 1) < LANES // 2
    for orb in range(n_orb):
        for ctile in range(n_aux // 2):
            blk = kacc[orb * row_pad:(orb + 1) * row_pad, ctile * LANES:(ctile + 1) * LANES]
            top, bot = blk[0:half], blk[half:]
            ksend[2 * ctile * n_orb + orb] = jnp.where(low_half, top, pltpu.roll(bot, LANES // 2, 1))
            ksend[(2 * ctile + 1) * n_orb + orb] = jnp.where(low_half, pltpu.roll(top, LANES // 2, 1), bot)
    dev = my * n_orb + me
    krecv[dev] = ksend[dev]

    def hops(step, ring):
        return min(step, ring - step)

    steps = [(ahead, flip, up) for ahead in range(n_chips) for flip in range(2) for up in range(n_aux)][1:]
    steps = sorted(steps, key=lambda p: -(hops(p[0], n_chips) + hops(p[2], n_aux)))

    def k_out(step):
        return k_copy(peer_at(step[:2]), lax.rem(my + step[2], n_aux), dev)

    for step in steps:
        k_out(step).start()
    for is_small, k in t_groups:
        for r in range(1, n_orb):
            t_copy(is_small, k, peer_orb(r), me).wait_send()
    for r in range(1, n_orb):
        l_copy(0, peer_orb(r), me).wait_send()
        if_last(peer_orb(r), l_copy(1, peer_orb(r), me).wait_send)
        g_copy(peer_orb(r), me).wait_send()
    for r in range(1, n_aux):
        j_copy(lax.rem(my + r, n_aux), my).wait_send()
    for r in range(1, n_aux):
        j_copy(my, lax.rem(my + r, n_aux)).wait_recv()
    jsum = jrecv[0]
    for src in range(1, n_aux):
        jsum = jsum + jrecv[src]

    for step in reversed(steps):
        k_copy(me, my, lax.rem(my + step[2], n_aux) * n_orb + peer_at(step[:2])).wait_recv()
    ksum = krecv[0]
    for src in range(1, n_dev):
        ksum = ksum + krecv[src]
    kblk = jnp.concatenate([ksum, pltpu.roll(ksum, LANES // 2, 1)], axis=0)
    pad_cols = row_pad - row_blk
    kcols = jnp.where(lax.broadcasted_iota(jnp.int32, (row_pad, LANES), 1) < row_blk, kblk, pltpu.roll(kblk, LANES - pad_cols, 1))
    out = 2.0 * jsum - kcols
    out_ref[...] = out[0:row_blk, 0:n_cols]

    for step in steps:
        k_out(step).wait_send()


def solution(mesh):
    n_orb = mesh.shape['orb']
    n_aux = mesh.shape['aux']

    def local_fock(fit_loc, orbitals):
        q_loc, row_blk, n_bf = fit_loc.shape
        n_occ = orbitals.shape[1]
        n_cols = n_bf // n_aux
        row_pad = rup(row_blk, SUBL)
        occ_each = n_occ // n_orb
        q_main = q_loc // LANES * LANES
        n_tiles = q_main // LANES
        slots = n_tiles * occ_each
        whole = row_blk // SUBL * SUBL
        left_pad = rup(q_loc - q_main, SUBL)
        fold = LANES // left_pad
        pairs = occ_each // fold
        extra = n_occ - n_orb * occ_each
        base = slots * row_blk
        rest = row_blk - whole
        assert n_orb == 2 * n_aux and n_cols == 2 * row_blk and occ_each % fold == 0 and occ_each < SUBL
        assert 0 < extra <= fold and (n_tiles + 1) * extra <= n_orb + 1 and row_pad * n_orb == 2 * LANES
        dims = (n_orb, n_aux, q_loc, row_blk, n_bf, n_occ, row_pad, occ_each, q_main, left_pad, fold, n_cols)
        n_dev = n_orb * n_aux
        n_groups = 1 + whole // SUBL
        assert len(ORDER) == n_orb - 1 and rest % SMALL_STEP == 0 and slots * rest % SUBL == 0 and slots % 2 == 0 and pairs == 2
        ex_rows = rup(pairs * row_blk, SUBL) + rup(row_blk, SUBL)
        q_lanes = rup(q_loc, LANES)
        g_rows = rup(q_lanes // LANES, 4)
        f32 = jnp.float32
        dma = pltpu.SemaphoreType.DMA
        scratch = [
            pltpu.VMEM((row_blk, q_loc, n_bf), f32),
            pltpu.VMEM((n_occ, n_bf), f32),
            pltpu.VMEM((n_bf, 2 * LANES), f32),
            pltpu.VMEM((row_blk, n_bf), f32),
            pltpu.VMEM((n_orb, base, LANES), f32),
            pltpu.VMEM((n_orb, base, LANES), f32),
            pltpu.VMEM((n_orb, ex_rows, LANES), f32),
            pltpu.VMEM((n_orb, ex_rows, LANES), f32),
            pltpu.VMEM((n_orb, row_pad, (slots + pairs + 2) * LANES), f32),
            pltpu.VMEM((n_orb * row_pad, n_orb * row_pad), f32),
            pltpu.VMEM((q_lanes, n_bf), f32),
            pltpu.VMEM((g_rows, LANES), f32),
            pltpu.VMEM((n_orb, g_rows, LANES), f32),
            pltpu.VMEM((q_lanes, n_bf), f32),
            pltpu.VMEM((row_pad, 2 * LANES), f32),
            pltpu.VMEM((n_aux, row_pad, LANES), f32),
            pltpu.VMEM((n_aux, row_pad, LANES), f32),
            pltpu.VMEM((n_dev, row_pad // 2, LANES), f32),
            pltpu.VMEM((n_dev, row_pad // 2, LANES), f32),
            dma((n_groups + 1,)), dma((n_groups, n_orb)), dma((n_groups, n_orb)), dma((2, n_orb)), dma((2, n_orb)),
            dma((n_orb,)), dma((n_orb,)), dma((n_aux,)), dma((n_aux,)), dma((n_dev,)), dma((n_dev,)),
        ]
        return pl.pallas_call(
            functools.partial(fock_kernel, dims),
            out_shape=jax.ShapeDtypeStruct((row_blk, n_cols), f32),
            in_specs=[pl.BlockSpec(memory_space=pltpu.HBM)] * 2,
            out_specs=pl.BlockSpec(memory_space=pltpu.VMEM),
            scratch_shapes=scratch,
            compiler_params=pltpu.CompilerParams(collective_id=0, has_side_effects=True, vmem_limit_bytes=32 * 1024 * 1024),
            name='fock_build',
        )(pltpu.with_memory_space_constraint(jnp.transpose(fit_loc, (1, 0, 2)), pltpu.HBM), pltpu.with_memory_space_constraint(orbitals.T, pltpu.HBM))

    spec_fit = P(('sys', 'aux'), 'orb', None)
    spec_orbitals = P('sys', None)
    spec_out = P(('sys', 'orb'), 'aux')
    return jax.shard_map(local_fock, mesh=mesh, in_specs=(spec_fit, spec_orbitals), out_specs=spec_out, check_vma=False)
```
